32 devices in a mesh: section: 4 (over y, x), tok: 8 (over z, core).
Axes of the slice: x: 2, y: 2, z: 4, core: 2. Of those that a mesh axis runs over, the one named last changes fastest.
Arguments:
- activations: bfloat16 [8, 2048, 8192], P('section', 'tok'), may hold values from -12 to 12
- projection: bfloat16 [8192, 512], P('tok'), may hold values from -0.0625 to 0.0625
Outputs:
- sketch: float32 [8, 512, 512], P('section', None, 'tok')
- similarity: float32 [8, 2], P('section')
The draws below stay inside these ranges and needn't reach their ends.
All inputs are finite; a program needn't handle non-finite values.
Results may differ from the reference program's by a relative error of at most 0.0003.
Values may be sent and summed in bfloat16 or wider, within the bound.
No kernel may reach another device: no remote copies, remote signals or barrier semaphores. Data moves between devices by JAX's collectives and lax.ppermute only.
A program may use at most 64 MiB of HBM per device.

```python
import jax
import jax.numpy as jnp
from jax import lax

D = 8192
RANK = 512
LAYERS = 8
TOKENS = 2048


def draw_activations(key, part):
    keyed = jax.random.fold_in(key, 11)
    key_base, key_weight, key_rows, key_mean, key_noise = jax.random.split(keyed, 5)
    shared = jax.random.normal(key_base, (TOKENS, D), jnp.float32)
    offset = jnp.zeros((D,), jnp.float32)
    mixing = jax.random.uniform(key_weight, (LAYERS,), jnp.float32, 0.2, 1.5)
    row_scale = jnp.exp(jax.random.uniform(key_rows, (LAYERS, TOKENS, 1), jnp.float32, jnp.log(0.3), jnp.log(3.0)))

    def one_layer(layer):
        noise = jax.random.normal(jax.random.fold_in(key_noise, layer), (TOKENS, D), jnp.float32)
        values = row_scale[layer] * (mixing[layer] * shared + noise) + offset
        return jnp.clip(values, -12.0, 12.0).astype(jnp.bfloat16)
    return lax.map(one_layer, jnp.arange(LAYERS, dtype=jnp.int32))


def block_levels(rng, shape, pieces, least, top_value):
    loudness, own = 1.0, jax.random.fold_in(rng, 6)
    for position, blocks in pieces:
        draws = jnp.exp(jax.random.uniform(jax.random.fold_in(own, position), (blocks,), jnp.float32, least / len(pieces), top_value / len(pieces)))
        loudness = loudness * jnp.repeat(draws, shape[position] // blocks).reshape([-1 if axis == position else 1 for axis in range(len(shape))])
    return loudness


def bell_draw(rng, shape, spread, most, cuts=(), held_as=jnp.bfloat16):
    level = block_levels(rng, shape, cuts, -0.22, 0.18) if cuts else 1.0
    drawn = jax.random.normal(rng, shape, jnp.float32) * spread * level
    return jnp.minimum(jnp.maximum(drawn, -most), most).astype(held_as)


def setup_inputs(seed: int = 0) -> dict:
    key_list = jax.random.split(jax.random.key(seed), 3)
    activations = draw_activations(jax.random.fold_in(key_list[2], 71), 0)
    projection = bell_draw(key_list[1], (D, RANK), D ** -0.5, 0.0625, ((0, 8),))
    return {"activations": activations, "projection": projection}


def reference(activations, projection):

    def layer_sketch(layer_acts):
        projected = jnp.dot(layer_acts, projection, preferred_element_type=jnp.float32)
        centred = projected - lax.optimization_barrier(jnp.sum(projected, axis=0)) / TOKENS
        return jnp.dot(centred.T, centred, precision=lax.Precision.HIGHEST)
    sketch = lax.map(layer_sketch, activations)
    flattened = sketch.reshape(sketch.shape[0], -1)
    squares = lax.optimization_barrier(jnp.sum(flattened * flattened, axis=1))
    before = jnp.concatenate([flattened[:1], flattened[:-1]], axis=0)
    beyond = jnp.concatenate([flattened[1:], flattened[-1:]], axis=0)
    square_before = jnp.concatenate([squares[:1], squares[:-1]])
    square_beyond = jnp.concatenate([squares[1:], squares[-1:]])
    earlier = lax.optimization_barrier(jnp.sum(flattened * before, axis=1)) / jnp.sqrt(squares * square_before)
    later = lax.optimization_barrier(jnp.sum(flattened * beyond, axis=1)) / jnp.sqrt(squares * square_beyond)
    return (sketch, jnp.stack([earlier, later], axis=1))
```

```python
import functools

import jax
import jax.numpy as jnp
from jax import lax
from jax.experimental import pallas as pl
from jax.experimental.pallas import tpu as pltpu
from jax.sharding import PartitionSpec as P


F32, BF16 = jnp.float32, jnp.bfloat16
SMEM = pl.BlockSpec(memory_space=pltpu.SMEM)
VMEM = pl.BlockSpec(memory_space=pltpu.VMEM)
ANY = pl.BlockSpec(memory_space=pl.ANY)


def swap(block, axis, mask):
    return lax.ppermute(block, axis, [(i, i ^ mask) for i in range(lax.axis_size(axis))])


def params(mib):
    return pltpu.CompilerParams(vmem_limit_bytes=mib << 20)


def cost(flops, moved):
    return pl.CostEstimate(flops=int(flops), bytes_accessed=int(moved), transcendentals=0)


def deal_kernel(width, pos, proj, mine, give):
    core = pos[1]
    rank, half = proj.shape[1], mine.shape[1]
    row = lax.broadcasted_iota(jnp.int32, (rank, half), 0)
    col = lax.broadcasted_iota(jnp.int32, (rank, half), 1)
    first = (col // width) * (2 * width) + col % width
    block = proj[...]
    for out, side in ((mine, core), (give, 1 - core)):
        pick = jnp.where(row == first + side * width, 1.0, 0.0).astype(BF16)
        out[...] = jnp.dot(block, pick, preferred_element_type=F32).astype(BF16)


def deal(pos, proj, width):
    rows, rank = proj.shape
    half = jax.ShapeDtypeStruct((rows, rank // 2), BF16)
    return pl.pallas_call(
        functools.partial(deal_kernel, width),
        out_shape=(half, half),
        in_specs=[SMEM, VMEM],
        out_specs=(VMEM, VMEM),
        compiler_params=params(12),
        cost_estimate=cost(2 * rows * rank * rank, 4 * rows * rank),
        name="deal",
    )(pos, proj)


def project_kernel(count, started, layers, offs, acts, other, *refs):
    pieces, refs = refs[:count], refs[count:]
    total = refs[0] if started else None
    refs = refs[started:]
    outs, (buf, sems) = refs[:-2], refs[-2:]
    copies = []
    for side, source in enumerate((acts, other)):
        at = 0
        for n, piece in enumerate(pieces):
            deep = piece.shape[0]
            src = source.at[:, pl.ds(pl.multiple_of(offs[n], 128), deep)]
            dst = buf.at[side, :, pl.ds(at, deep)]
            copy = pltpu.make_async_copy(src, dst, sems.at[side, n])
            copy.start()
            copies.append(copy)
            at += deep
    weights = jnp.concatenate([piece[...] for piece in pieces], axis=0)
    rows = acts.shape[0] // layers
    kept = []
    for side in range(2):
        for copy in copies[side * count : (side + 1) * count]:
            copy.wait()
        for layer in range(layers):
            span = pl.ds(layer * rows, rows)
            part = jnp.dot(buf[side, span, :], weights, preferred_element_type=F32)
            if started:
                part = part + total[side, span, :]
            if len(outs) == 1:
                outs[0][side, span, :] = part
            else:
                kept.append(part)
    if len(outs) == 1:
        return
    split, sums = outs
    sums[...] = jnp.zeros_like(sums)
    for layer in range(layers):
        parts = [kept[layer], kept[layers + layer]]
        column = jnp.sum(parts[0] + parts[1], axis=0, keepdims=True)
        sums[layer : layer + 1, :] = column
        mean = column / (2 * rows)
        for side in range(2):
            span = pl.ds(layer * rows, rows)
            value = parts[side] - mean
            high = value.astype(BF16)
            split[0, side, span, :] = high
            split[1, side, span, :] = (value - high.astype(F32)).astype(BF16)


def project(pieces, offs, total, acts, other, layers, last):
    rows, half = acts.shape[0], pieces[0].shape[1]
    deep = sum(piece.shape[0] for piece in pieces)
    if last:
        out_shape = (
            jax.ShapeDtypeStruct((2, 2, rows, half), BF16),
            jax.ShapeDtypeStruct((8, half), F32),
        )
        out_specs = (VMEM, VMEM)
    else:
        out_shape = jax.ShapeDtypeStruct((2, rows, half), F32)
        out_specs = VMEM
    started = [] if total is None else [total]
    return pl.pallas_call(
        functools.partial(project_kernel, len(pieces), len(started), layers),
        out_shape=out_shape,
        in_specs=[SMEM, ANY, ANY] + [VMEM] * (len(pieces) + len(started)),
        out_specs=out_specs,
        scratch_shapes=[
            pltpu.VMEM((2, rows, deep), BF16),
            pltpu.SemaphoreType.DMA((2, len(pieces))),
        ],
        compiler_params=params(20),
        cost_estimate=cost(4 * rows * deep * half, 4 * rows * deep),
        name="project",
    )(offs, acts, other, *pieces, *started)


def gram_kernel(layers, chips, pos, own, oth, own_sums, oth_sums, *outs):
    chip = pos[0]
    half = own.shape[3]
    rows = own.shape[2] // layers
    width = half // chips
    along_tokens = (((0,), (0,)), ((), ()))
    for layer in range(layers):
        span = pl.ds(layer * rows, rows)
        left, right = [], []
        for part in range(2):
            here = jnp.concatenate([own[part, 0, span, :], own[part, 1, span, :]], axis=0)
            there = jnp.concatenate([oth[part, 1, span, :], oth[part, 0, span, :]], axis=0)
            left.append(here)
            right.append(jnp.concatenate([here, there], axis=1))
        gram = sum(
            lax.dot_general(left[i], right[j], along_tokens, preferred_element_type=F32)
            for i, j in ((0, 0), (0, 1), (1, 0))
        )
        blocks = [gram[i * width : (i + 1) * width] for i in range(chips)]
        for k, out in enumerate(outs):
            block = blocks[k]
            for i in range(1, chips):
                block = jnp.where(chip == i, blocks[i ^ k], block)
            out[layer * width : (layer + 1) * width, :] = block
    sums = jnp.concatenate([own_sums[...], oth_sums[...]], axis=1)
    for out in outs:
        out[layers * width :, :] = sums


def gram(pos, own, oth, own_sums, oth_sums, layers, chips):
    rows, half = own.shape[2:]
    message = jax.ShapeDtypeStruct((layers * (half // chips) + 8, 2 * half), F32)
    return pl.pallas_call(
        functools.partial(gram_kernel, layers, chips),
        out_shape=(message,) * chips,
        in_specs=[SMEM] + [VMEM] * 4,
        out_specs=(VMEM,) * chips,
        compiler_params=params(16),
        cost_estimate=cost(24 * rows * half * half, 16 * rows * half),
        name="gram",
    )(pos, own, oth, own_sums, oth_sums)


def finish_kernel(layers, chips, tokens, pos, *refs):
    messages, (sketch, turned, first_out, second_out) = refs[:chips], refs[chips:]
    chip, core, section = pos[0], pos[1], pos[2]
    rank = messages[0].shape[1]
    width = (messages[0].shape[0] - 8) // layers
    half = rank // 2
    here = lax.broadcasted_iota(jnp.int32, (width, rank), 1)
    here = here == lax.broadcasted_iota(jnp.int32, (width, rank), 0) + chip * width
    kept = []
    for layer in range(layers):
        span = slice(layer * width, (layer + 1) * width)
        value = sum(message[span, :] for message in messages[1:]) + messages[0][span, :]
        at = layers * width + layer
        sums = [message[at : at + 1, :] for message in messages]
        mean = sum(sums) / tokens
        for total in sums:
            drift = total / (tokens // chips) - mean
            lifted = jnp.sum(jnp.where(here, drift, 0.0), axis=1, keepdims=True)
            value = value + (tokens // chips) * lifted * drift
        turned[layer] = value
        kept.append(value)
        flipped = value.T
        for i in range(chips):
            for side in range(2):
                at = side * half + i * width
                to = 2 * width * i + width * (core if side == 0 else 1 - core)
                rows = pl.ds(pl.multiple_of(to, 8), width)
                sketch[layer, rows, :] = flipped[at : at + width]
    odd = section % 2 == 1
    first_out[...] = jnp.where(odd, kept[0], kept[-1]).astype(BF16)
    second_out[...] = jnp.where(odd, kept[-1], kept[0]).astype(BF16)


def finish(pos, messages, layers, tokens):
    rank = messages[0].shape[1]
    width = (messages[0].shape[0] - 8) // layers
    edge = jax.ShapeDtypeStruct((width, rank), BF16)
    return pl.pallas_call(
        functools.partial(finish_kernel, layers, len(messages), tokens),
        out_shape=(
            jax.ShapeDtypeStruct((layers, rank, width), F32),
            jax.ShapeDtypeStruct((layers, width, rank), F32),
            edge,
            edge,
        ),
        in_specs=[SMEM] + [VMEM] * len(messages),
        out_specs=(VMEM,) * 4,
        compiler_params=params(12),
        cost_estimate=cost(1e6, 2e6),
        name="finish",
    )(pos, *messages)


def products_kernel(layers, sections, pos, turned, one, two, out):
    section = pos[2]
    odd = section % 2 == 1
    one, two = one[...].astype(F32), two[...].astype(F32)
    rows = [turned[i] for i in range(layers)]
    before = jnp.where(section == 0, rows[0], jnp.where(odd, one, two))
    beyond = jnp.where(section == sections - 1, rows[-1], jnp.where(odd, two, one))
    pairs = [(before, before)] + [(row, row) for row in rows] + [(beyond, beyond)]
    chain = [before] + rows + [beyond]
    pairs += list(zip(chain[:-1], chain[1:]))
    out[...] = jnp.zeros_like(out)
    for n, (a, b) in enumerate(pairs):
        out[n : n + 1, :] = jnp.full((1, out.shape[1]), jnp.sum(a * b), F32)


def products(pos, turned, one, two, sections):
    layers = turned.shape[0]
    count = -(-(2 * layers + 3) // 8) * 8
    return pl.pallas_call(
        functools.partial(products_kernel, layers, sections),
        out_shape=jax.ShapeDtypeStruct((count, 128), F32),
        in_specs=[SMEM] + [VMEM] * 3,
        out_specs=VMEM,
        compiler_params=params(4),
        cost_estimate=cost(1e6, 1e6),
        name="products",
    )(pos, turned, one, two)


def ratios_kernel(layers, one, two, out):
    value = one[...] + two[...]
    squares = value[: layers + 2]
    chained = value[layers + 2 : 2 * layers + 3]
    ratio = chained / jnp.sqrt(squares[:-1] * squares[1:])
    out[:, 0:1] = ratio[:-1, 0:1]
    out[:, 1:2] = ratio[1:, 0:1]


def ratios(one, two, layers):
    return pl.pallas_call(
        functools.partial(ratios_kernel, layers),
        out_shape=jax.ShapeDtypeStruct((layers, 2), F32),
        in_specs=[VMEM] * 2,
        out_specs=VMEM,
        compiler_params=params(4),
        cost_estimate=cost(1e4, 1e4),
        name="ratios",
    )(one, two)


def local(activations, projection):
    layers, tok_rows, model = activations.shape
    block, rank = projection.shape
    groups, sections = lax.axis_size("tok"), lax.axis_size("section")
    chips, width = groups // 2, rank // groups
    tok, section = lax.axis_index("tok"), lax.axis_index("section")
    chip, core = tok // 2, tok % 2
    pos = jnp.stack([chip, core, section]).astype(jnp.int32)
    parts = min(sections, max(1, block // 128))
    deep = block // parts

    acts = activations.reshape(layers * tok_rows, model)
    mine, give = deal(pos, projection, width)
    got = swap(give, "tok", 1)
    other = swap(acts, "tok", 1)
    start = (section % parts) * deep
    share = jnp.stack([lax.dynamic_slice_in_dim(x, start, deep, 0) for x in (mine, got)])
    share = share.reshape(2 * deep, rank // 2)

    fetched = {}
    for k in range(1, chips):
        low = k & -k
        fetched[k] = swap(share if k == low else fetched[k ^ low], "tok", 2 * low)

    offs = jnp.stack([tok * block, (tok ^ 1) * block]).astype(jnp.int32)
    total = project([mine, got], offs, None, acts, other, layers, False)
    order = sorted(fetched, key=lambda k: (bin(k).count("1"), k))
    for k in order:
        pieces = [fetched[k]] + [swap(fetched[k], "section", j) for j in range(1, parts)]
        halves, offs = [], []
        for j, piece in enumerate(pieces):
            for side in range(2):
                halves.append(piece[side * deep : (side + 1) * deep])
                offs.append((tok ^ (2 * k + side)) * block + ((section % parts) ^ j) * deep)
        offs = jnp.stack(offs).astype(jnp.int32)
        total = project(halves, offs, total, acts, other, layers, k == order[-1])
    split, sums = total

    messages = gram(pos, split, swap(split, "tok", 1), sums, swap(sums, "tok", 1), layers, chips)
    arrived = [messages[0]]
    for k in reversed(range(1, chips)):
        arrived.append(swap(messages[k], "tok", 2 * k))
    sketch, turned, first, second = finish(pos, arrived, layers, tok_rows * groups)

    first = swap(first, "section", 1)
    route = [(i, i + 1) for i in range(1, sections - 1, 2)]
    second = lax.ppermute(second, "section", route + [(b, a) for a, b in route])
    value = products(pos, turned, first, second, sections)
    mask = 1
    while 2 * mask < groups:
        value = value + swap(value, "tok", mask)
        mask *= 2
    return sketch, ratios(value, swap(value, "tok", mask), layers)


def solution(mesh):
    return jax.shard_map(
        local,
        mesh=mesh,
        in_specs=(P("section", "tok", None), P("tok", None)),
        out_specs=(P("section", None, "tok"), P("section", None)),
        check_vma=False,
    )
```

```python
import functools

import jax
import jax.numpy as jnp
from jax import lax
from jax.experimental import pallas as pl
from jax.experimental.pallas import tpu as pltpu
from jax.sharding import PartitionSpec as P


F32, BF16 = jnp.float32, jnp.bfloat16
SMEM = pl.BlockSpec(memory_space=pltpu.SMEM)
VMEM = pl.BlockSpec(memory_space=pltpu.VMEM)
ANY = pl.BlockSpec(memory_space=pl.ANY)


def swap(block, axis, mask):
    return lax.ppermute(block, axis, [(i, i ^ mask) for i in range(lax.axis_size(axis))])


def params(mib):
    return pltpu.CompilerParams(vmem_limit_bytes=mib << 20)


def cost(flops, moved):
    return pl.CostEstimate(flops=int(flops), bytes_accessed=int(moved), transcendentals=0)


def deal_kernel(width, pos, proj, mine, give):
    core = pos[1]
    rank, half = proj.shape[1], mine.shape[1]
    row = lax.broadcasted_iota(jnp.int32, (rank, half), 0)
    col = lax.broadcasted_iota(jnp.int32, (rank, half), 1)
    first = (col // width) * (2 * width) + col % width
    block = proj[...]
    for out, side in ((mine, core), (give, 1 - core)):
        pick = jnp.where(row == first + side * width, 1.0, 0.0).astype(BF16)
        out[...] = jnp.dot(block, pick, preferred_element_type=F32).astype(BF16)


def deal(pos, proj, width):
    rows, rank = proj.shape
    half = jax.ShapeDtypeStruct((rows, rank // 2), BF16)
    return pl.pallas_call(
        functools.partial(deal_kernel, width),
        out_shape=(half, half),
        in_specs=[SMEM, VMEM],
        out_specs=(VMEM, VMEM),
        compiler_params=params(12),
        cost_estimate=cost(2 * rows * rank * rank, 4 * rows * rank),
        name="deal",
    )(pos, proj)


def stage_kernel(parts, offs, source, *refs):
    outs, sems = refs[:-1], refs[-1]
    copies = []
    for n, out in enumerate(outs):
        deep = out.shape[1] // parts
        for i in range(parts):
            off = pl.multiple_of(offs[n * parts + i], 128)
            src, dst = source.at[:, pl.ds(off, deep)], out.at[:, pl.ds(i * deep, deep)]
            copies.append(pltpu.make_async_copy(src, dst, sems.at[n, i]))
            copies[-1].start()
    for copy in copies:
        copy.wait()


def stage(offs, source, parts, deep):
    count, rows = len(offs), source.shape[0]
    out = jax.ShapeDtypeStruct((rows, parts * deep), BF16)
    return pl.pallas_call(
        functools.partial(stage_kernel, parts),
        out_shape=(out,) * count,
        in_specs=[SMEM, ANY],
        out_specs=(VMEM,) * count,
        scratch_shapes=[pltpu.SemaphoreType.DMA((count, parts))],
        compiler_params=params(48),
        cost_estimate=cost(4e9, 4 * rows * parts * deep * count),
        name="stage",
    )(jnp.concatenate(offs), source)


def project_kernel(count, started, layers, acts, other, *refs):
    pieces, refs = refs[:count], refs[count:]
    total = refs[0] if started else None
    outs = refs[started:]
    weights = jnp.concatenate([piece[...] for piece in pieces], axis=0)
    rows = acts.shape[0] // layers
    kept = []
    for side, source in enumerate((acts, other)):
        for layer in range(layers):
            span = pl.ds(layer * rows, rows)
            part = jnp.dot(source[span, :], weights, preferred_element_type=F32)
            if started:
                part = part + total[side, span, :]
            if len(outs) == 1:
                outs[0][side, span, :] = part
            else:
                kept.append(part)
    if len(outs) == 1:
        return
    split, sums = outs
    sums[...] = jnp.zeros_like(sums)
    for layer in range(layers):
        parts = [kept[layer], kept[layers + layer]]
        column = jnp.sum(parts[0] + parts[1], axis=0, keepdims=True)
        sums[layer : layer + 1, :] = column
        mean = column / (2 * rows)
        for side in range(2):
            span = pl.ds(layer * rows, rows)
            value = parts[side] - mean
            high = value.astype(BF16)
            split[0, side, span, :] = high
            split[1, side, span, :] = (value - high.astype(F32)).astype(BF16)


def project(pieces, total, acts, other, layers, last):
    rows, half = acts.shape[0], pieces[0].shape[1]
    deep = sum(piece.shape[0] for piece in pieces)
    if last:
        out_shape = (
            jax.ShapeDtypeStruct((2, 2, rows, half), BF16),
            jax.ShapeDtypeStruct((8, half), F32),
        )
        out_specs = (VMEM, VMEM)
    else:
        out_shape = jax.ShapeDtypeStruct((2, rows, half), F32)
        out_specs = VMEM
    started = [] if total is None else [total]
    return pl.pallas_call(
        functools.partial(project_kernel, len(pieces), len(started), layers),
        out_shape=out_shape,
        in_specs=[VMEM] * (2 + len(pieces) + len(started)),
        out_specs=out_specs,
        compiler_params=params(16),
        cost_estimate=cost(4 * rows * deep * half, 4 * rows * deep),
        name="project",
    )(acts, other, *pieces, *started)


def gram_kernel(layers, chips, pos, own, oth, own_sums, oth_sums, *outs):
    chip = pos[0]
    half = own.shape[3]
    rows = own.shape[2] // layers
    width = half // chips
    along_tokens = (((0,), (0,)), ((), ()))
    for layer in range(layers):
        span = pl.ds(layer * rows, rows)
        left, right = [], []
        for part in range(2):
            here = jnp.concatenate([own[part, 0, span, :], own[part, 1, span, :]], axis=0)
            there = jnp.concatenate([oth[part, 1, span, :], oth[part, 0, span, :]], axis=0)
            left.append(here)
            right.append(jnp.concatenate([here, there], axis=1))
        gram = sum(
            lax.dot_general(left[i], right[j], along_tokens, preferred_element_type=F32)
            for i, j in ((0, 0), (0, 1), (1, 0))
        )
        blocks = [gram[i * width : (i + 1) * width] for i in range(chips)]
        for k, out in enumerate(outs):
            block = blocks[k]
            for i in range(1, chips):
                block = jnp.where(chip == i, blocks[i ^ k], block)
            out[layer * width : (layer + 1) * width, :] = block
    sums = jnp.concatenate([own_sums[...], oth_sums[...]], axis=1)
    for out in outs:
        out[layers * width :, :] = sums


def gram(pos, own, oth, own_sums, oth_sums, layers, chips):
    rows, half = own.shape[2:]
    message = jax.ShapeDtypeStruct((layers * (half // chips) + 8, 2 * half), F32)
    return pl.pallas_call(
        functools.partial(gram_kernel, layers, chips),
        out_shape=(message,) * chips,
        in_specs=[SMEM] + [VMEM] * 4,
        out_specs=(VMEM,) * chips,
        compiler_params=params(16),
        cost_estimate=cost(24 * rows * half * half, 16 * rows * half),
        name="gram",
    )(pos, own, oth, own_sums, oth_sums)


def finish_kernel(layers, chips, tokens, pos, *refs):
    messages, (sketch, turned, first_out, second_out) = refs[:chips], refs[chips:]
    chip, core, section = pos[0], pos[1], pos[2]
    rank = messages[0].shape[1]
    width = (messages[0].shape[0] - 8) // layers
    half = rank // 2
    here = lax.broadcasted_iota(jnp.int32, (width, rank), 1)
    here = here == lax.broadcasted_iota(jnp.int32, (width, rank), 0) + chip * width
    kept = []
    for layer in range(layers):
        span = slice(layer * width, (layer + 1) * width)
        value = sum(message[span, :] for message in messages[1:]) + messages[0][span, :]
        at = layers * width + layer
        sums = [message[at : at + 1, :] for message in messages]
        mean = sum(sums) / tokens
        for total in sums:
            drift = total / (tokens // chips) - mean
            lifted = jnp.sum(jnp.where(here, drift, 0.0), axis=1, keepdims=True)
            value = value + (tokens // chips) * lifted * drift
        turned[layer] = value
        kept.append(value)
        flipped = value.T
        for i in range(chips):
            for side in range(2):
                at = side * half + i * width
                to = 2 * width * i + width * (core if side == 0 else 1 - core)
                rows = pl.ds(pl.multiple_of(to, 8), width)
                sketch[layer, rows, :] = flipped[at : at + width]
    odd = section % 2 == 1
    first_out[...] = jnp.where(odd, kept[0], kept[-1]).astype(BF16)
    second_out[...] = jnp.where(odd, kept[-1], kept[0]).astype(BF16)


def finish(pos, messages, layers, tokens):
    rank = messages[0].shape[1]
    width = (messages[0].shape[0] - 8) // layers
    edge = jax.ShapeDtypeStruct((width, rank), BF16)
    return pl.pallas_call(
        functools.partial(finish_kernel, layers, len(messages), tokens),
        out_shape=(
            jax.ShapeDtypeStruct((layers, rank, width), F32),
            jax.ShapeDtypeStruct((layers, width, rank), F32),
            edge,
            edge,
        ),
        in_specs=[SMEM] + [VMEM] * len(messages),
        out_specs=(VMEM,) * 4,
        compiler_params=params(12),
        cost_estimate=cost(1e6, 2e6),
        name="finish",
    )(pos, *messages)


def products_kernel(layers, sections, pos, turned, one, two, out):
    section = pos[2]
    odd = section % 2 == 1
    one, two = one[...].astype(F32), two[...].astype(F32)
    rows = [turned[i] for i in range(layers)]
    before = jnp.where(section == 0, rows[0], jnp.where(odd, one, two))
    beyond = jnp.where(section == sections - 1, rows[-1], jnp.where(odd, two, one))
    pairs = [(before, before)] + [(row, row) for row in rows] + [(beyond, beyond)]
    chain = [before] + rows + [beyond]
    pairs += list(zip(chain[:-1], chain[1:]))
    out[...] = jnp.zeros_like(out)
    for n, (a, b) in enumerate(pairs):
        out[n : n + 1, :] = jnp.full((1, out.shape[1]), jnp.sum(a * b), F32)


def products(pos, turned, one, two, sections):
    layers = turned.shape[0]
    count = -(-(2 * layers + 3) // 8) * 8
    return pl.pallas_call(
        functools.partial(products_kernel, layers, sections),
        out_shape=jax.ShapeDtypeStruct((count, 128), F32),
        in_specs=[SMEM] + [VMEM] * 3,
        out_specs=VMEM,
        compiler_params=params(4),
        cost_estimate=cost(1e6, 1e6),
        name="products",
    )(pos, turned, one, two)


def ratios_kernel(layers, one, two, out):
    value = one[...] + two[...]
    squares = value[: layers + 2]
    chained = value[layers + 2 : 2 * layers + 3]
    ratio = chained / jnp.sqrt(squares[:-1] * squares[1:])
    out[:, 0:1] = ratio[:-1, 0:1]
    out[:, 1:2] = ratio[1:, 0:1]


def ratios(one, two, layers):
    return pl.pallas_call(
        functools.partial(ratios_kernel, layers),
        out_shape=jax.ShapeDtypeStruct((layers, 2), F32),
        in_specs=[VMEM] * 2,
        out_specs=VMEM,
        compiler_params=params(4),
        cost_estimate=cost(1e4, 1e4),
        name="ratios",
    )(one, two)


def local(activations, projection):
    layers, tok_rows, model = activations.shape
    block, rank = projection.shape
    groups, sections = lax.axis_size("tok"), lax.axis_size("section")
    chips, width = groups // 2, rank // groups
    tok, section = lax.axis_index("tok"), lax.axis_index("section")
    chip, core = tok // 2, tok % 2
    pos = jnp.stack([chip, core, section]).astype(jnp.int32)
    parts = min(sections, max(1, block // 128))
    deep = block // parts

    acts = activations.reshape(layers * tok_rows, model)
    mine, give = deal(pos, projection, width)
    got = swap(give, "tok", 1)
    other = swap(acts, "tok", 1)

    def share(j):
        start = ((section % parts) ^ j) * deep
        pair = [lax.dynamic_slice_in_dim(x, start, deep, 0) for x in (mine, got)]
        return jnp.concatenate(pair, axis=0)

    own, fetched = share(0), {}
    for k in range(1, chips):
        low = k & -k
        fetched[k] = swap(own if k == low else fetched[k ^ low], "tok", 2 * low)

    def places(k):
        spots = []
        for j in range(parts):
            at = ((section % parts) ^ j) * deep
            spots += [(tok ^ (2 * k + side)) * block + at for side in range(2)]
        return jnp.stack(spots).astype(jnp.int32)

    both = jnp.stack([tok, tok ^ 1]).astype(jnp.int32) * block
    both = (both[:, None] + jnp.arange(parts, dtype=jnp.int32) * deep).reshape(-1)
    order = sorted(fetched, key=lambda k: (bin(k).count("1"), -k))
    early, late = [0, order[-1]], order[:-1]
    spots = {k: places(k) for k in order} | {0: both}
    staged = {k: [] for k in spots}
    for source in (acts, other):
        for keys in (early, late):
            if keys:
                for k, out in zip(keys, stage([spots[k] for k in keys], source, 2 * parts, deep)):
                    staged[k].append(out)

    total = project([mine, got], None, *staged[0], layers, False)
    for k in order:
        pieces = [fetched[k]]
        for j in range(1, parts):
            if k == 1 and j & (j - 1):
                pieces.append(swap(share(j), "tok", 2))
            else:
                pieces.append(swap(fetched[k], "section", j))
        total = project(pieces, total, *staged[k], layers, k == order[-1])
    split, sums = total

    messages = gram(pos, split, swap(split, "tok", 1), sums, swap(sums, "tok", 1), layers, chips)
    arrived = [messages[0]]
    for k in reversed(range(1, chips)):
        arrived.append(swap(messages[k], "tok", 2 * k))
    sketch, turned, first, second = finish(pos, arrived, layers, tok_rows * groups)

    first = swap(first, "section", 1)
    route = [(i, i + 1) for i in range(1, sections - 1, 2)]
    second = lax.ppermute(second, "section", route + [(b, a) for a, b in route])
    value = products(pos, turned, first, second, sections)
    mask = 1
    while 2 * mask < groups:
        value = value + swap(value, "tok", mask)
        mask *= 2
    return sketch, ratios(value, swap(value, "tok", mask), layers)


def solution(mesh):
    return jax.shard_map(
        local,
        mesh=mesh,
        in_specs=(P("section", "tok", None), P("tok", None)),
        out_specs=(P("section", None, "tok"), P("section", None)),
        check_vma=False,
    )
```

```python
import functools

import jax
import jax.numpy as jnp
from jax import lax
from jax.experimental import pallas as pl
from jax.experimental.pallas import tpu as pltpu
from jax.sharding import PartitionSpec as P


F32, BF16 = jnp.float32, jnp.bfloat16
SMEM = pl.BlockSpec(memory_space=pltpu.SMEM)
VMEM = pl.BlockSpec(memory_space=pltpu.VMEM)
HBM = pl.BlockSpec(memory_space=pltpu.HBM)


def swap(block, axis, mask):
    return lax.ppermute(block, axis, [(i, i ^ mask) for i in range(lax.axis_size(axis))])


def params(mib):
    return pltpu.CompilerParams(vmem_limit_bytes=int(mib * 1024) << 10)


def cost(flops, moved):
    return pl.CostEstimate(flops=int(flops), bytes_accessed=int(moved), transcendentals=0)


def deal_kernel(width, rows, pos, proj, mine, give, block, sem):
    core, section = pos[1], pos[2]
    start = 0
    if rows < proj.shape[0]:
        start = pl.multiple_of((section % (proj.shape[0] // rows)) * rows, 16)
    copy = pltpu.make_async_copy(proj.at[pl.ds(start, rows), :], block, sem)
    copy.start()
    rank, half = proj.shape[1], mine.shape[1]
    row = lax.broadcasted_iota(jnp.int32, (rank, half), 0)
    col = lax.broadcasted_iota(jnp.int32, (rank, half), 1)
    first = (col // width) * (2 * width) + col % width
    picks = [
        jnp.where(row == first + side * width, 1.0, 0.0).astype(BF16) for side in (core, 1 - core)
    ]
    copy.wait()
    for out, pick in zip((mine, give), picks):
        out[...] = jnp.dot(block[...], pick, preferred_element_type=F32).astype(BF16)


def deal(pos, proj, width, rows):
    rank = proj.shape[1]
    half = jax.ShapeDtypeStruct((rows, rank // 2), BF16)
    return pl.pallas_call(
        functools.partial(deal_kernel, width, rows),
        out_shape=(half, half),
        in_specs=[SMEM, HBM],
        out_specs=(VMEM, VMEM),
        scratch_shapes=[pltpu.VMEM((rows, rank), BF16), pltpu.SemaphoreType.DMA],
        compiler_params=params(4 if rows == proj.shape[0] else 63.25),
        cost_estimate=cost(2 * rows * rank * rank, 4 * rows * rank),
        name="deal",
    )(pos, proj)


def stage_kernel(k, pos, source, out, sem):
    deep = out.shape[1]
    columns = pl.ds(pl.multiple_of((pos[0] ^ k) * deep, 128), deep)
    copy = pltpu.make_async_copy(source.at[:, columns], out, sem)
    copy.start()
    copy.wait()


def stage(pos, source, k, deep):
    rows = source.shape[0]
    return pl.pallas_call(
        functools.partial(stage_kernel, k),
        out_shape=jax.ShapeDtypeStruct((rows, deep), BF16),
        in_specs=[SMEM, HBM],
        out_specs=VMEM,
        scratch_shapes=[pltpu.SemaphoreType.DMA],
        compiler_params=params(3),
        cost_estimate=cost(4e9, 4 * rows * deep),
        name="stage",
    )(pos, source)


def join_kernel(upper, lower, out):
    deep = upper.shape[0]
    out[:deep, :] = upper[...]
    out[deep:, :] = lower[...]


def join(upper, lower):
    deep, half = upper.shape
    return pl.pallas_call(
        join_kernel,
        out_shape=jax.ShapeDtypeStruct((2 * deep, half), BF16),
        in_specs=[VMEM, VMEM],
        out_specs=VMEM,
        compiler_params=params(2),
        cost_estimate=cost(1e6, 8 * deep * half),
        name="join",
    )(upper, lower)


def pick_kernel(parts, j, pos, upper, lower, out):
    deep = out.shape[0] // 2
    rows = pl.ds(pl.multiple_of(((pos[2] % parts) ^ j) * deep, 16), deep)
    out[:deep, :] = upper[rows, :]
    out[deep:, :] = lower[rows, :]


def pick(pos, upper, lower, parts, j):
    rows, half = upper.shape
    return pl.pallas_call(
        functools.partial(pick_kernel, parts, j),
        out_shape=jax.ShapeDtypeStruct((2 * rows // parts, half), BF16),
        in_specs=[SMEM, VMEM, VMEM],
        out_specs=VMEM,
        compiler_params=params(4),
        cost_estimate=cost(1e6, 8 * rows * half // parts),
        name="pick",
    )(pos, upper, lower)


def project_kernel(count, parts, started, layers, pos, acts, other, *refs):
    pieces, refs = refs[:count], refs[count:]
    total = refs[0] if started else None
    outs, weights = refs[started:-1], refs[-1]
    core, part = pos[1], pos[2] % parts
    block = weights.shape[0] // 2
    if count == 2:
        for piece, side in zip(pieces, (core, 1 - core)):
            weights[pl.ds(pl.multiple_of(side * block, 16), block), :] = piece[...]
    else:
        deep = block // parts
        for j, piece in enumerate(pieces):
            for n, side in enumerate((core, 1 - core)):
                at = pl.multiple_of(side * block + (part ^ j) * deep, 16)
                weights[pl.ds(at, deep), :] = piece[n * deep : (n + 1) * deep, :]
    rows = acts.shape[0] // layers
    kept = []
    for side, source in enumerate((acts, other)):
        for layer in range(layers):
            span = pl.ds(layer * rows, rows)
            value = jnp.dot(source[span, :], weights[...], preferred_element_type=F32)
            if started:
                value = value + total[side, span, :]
            if len(outs) == 1:
                outs[0][side, span, :] = value
            else:
                kept.append(value)
    if len(outs) == 1:
        return
    split, sums = outs
    sums[...] = jnp.zeros_like(sums)
    for layer in range(layers):
        values = [kept[layer], kept[layers + layer]]
        column = jnp.sum(values[0] + values[1], axis=0, keepdims=True)
        sums[layer : layer + 1, :] = column
        mean = column / (2 * rows)
        for side in range(2):
            span = pl.ds(layer * rows, rows)
            value = values[side] - mean
            high = value.astype(BF16)
            split[0, side, span, :] = high
            split[1, side, span, :] = (value - high.astype(F32)).astype(BF16)


def project(pos, pieces, parts, total, acts, other, layers, last):
    rows, deep = acts.shape
    half = pieces[0].shape[1]
    if last:
        out_shape = (
            jax.ShapeDtypeStruct((2, 2, rows, half), BF16),
            jax.ShapeDtypeStruct((8, half), F32),
        )
        out_specs = (VMEM, VMEM)
    else:
        out_shape = jax.ShapeDtypeStruct((2, rows, half), F32)
        out_specs = VMEM
    started = [] if total is None else [total]
    return pl.pallas_call(
        functools.partial(project_kernel, len(pieces), parts, len(started), layers),
        out_shape=out_shape,
        in_specs=[SMEM] + [VMEM] * (2 + len(pieces) + len(started)),
        out_specs=out_specs,
        scratch_shapes=[pltpu.VMEM((deep, half), BF16)],
        compiler_params=params(10),
        cost_estimate=cost(4 * rows * deep * half, 4 * rows * deep),
        name="project",
    )(pos, acts, other, *pieces, *started)


def gram_kernel(layers, chips, pos, own, oth, own_sums, oth_sums, *outs):
    chip = pos[0]
    half = own.shape[3]
    rows = own.shape[2] // layers
    width = half // chips
    along_tokens = (((0,), (0,)), ((), ()))
    for layer in range(layers):
        span = pl.ds(layer * rows, rows)
        left, right = [], []
        for part in range(2):
            here = jnp.concatenate([own[part, 0, span, :], own[part, 1, span, :]], axis=0)
            there = jnp.concatenate([oth[part, 1, span, :], oth[part, 0, span, :]], axis=0)
            left.append(here)
            right.append(jnp.concatenate([here, there], axis=1))
        gram = sum(
            lax.dot_general(left[i], right[j], along_tokens, preferred_element_type=F32)
            for i, j in ((0, 0), (0, 1), (1, 0))
        )
        blocks = [gram[i * width : (i + 1) * width] for i in range(chips)]
        for k, out in enumerate(outs):
            block = blocks[k]
            for i in range(1, chips):
                block = jnp.where(chip == i, blocks[i ^ k], block)
            out[layer * width : (layer + 1) * width, :] = block
    sums = jnp.concatenate([own_sums[...], oth_sums[...]], axis=1)
    for out in outs:
        out[layers * width :, :] = sums


def gram(pos, own, oth, own_sums, oth_sums, layers, chips):
    rows, half = own.shape[2:]
    message = jax.ShapeDtypeStruct((layers * (half // chips) + 8, 2 * half), F32)
    return pl.pallas_call(
        functools.partial(gram_kernel, layers, chips),
        out_shape=(message,) * chips,
        in_specs=[SMEM] + [VMEM] * 4,
        out_specs=(VMEM,) * chips,
        compiler_params=params(10),
        cost_estimate=cost(24 * rows * half * half, 16 * rows * half),
        name="gram",
    )(pos, own, oth, own_sums, oth_sums)


def finish_kernel(layers, chips, tokens, pos, *refs):
    messages, (sketch, turned, first_out, second_out) = refs[:chips], refs[chips:]
    chip, core, section = pos[0], pos[1], pos[2]
    rank = messages[0].shape[1]
    width = (messages[0].shape[0] - 8) // layers
    half = rank // 2
    here = lax.broadcasted_iota(jnp.int32, (width, rank), 1)
    here = here == lax.broadcasted_iota(jnp.int32, (width, rank), 0) + chip * width
    kept = []
    for layer in range(layers):
        span = slice(layer * width, (layer + 1) * width)
        value = sum(message[span, :] for message in messages[1:]) + messages[0][span, :]
        at = layers * width + layer
        sums = [message[at : at + 1, :] for message in messages]
        mean = sum(sums) / tokens
        for total in sums:
            drift = total / (tokens // chips) - mean
            lifted = jnp.sum(jnp.where(here, drift, 0.0), axis=1, keepdims=True)
            value = value + (tokens // chips) * lifted * drift
        turned[layer] = value
        kept.append(value)
        flipped = value.T
        for i in range(chips):
            for side in range(2):
                at = side * half + i * width
                to = 2 * width * i + width * (core if side == 0 else 1 - core)
                rows = pl.ds(pl.multiple_of(to, 8), width)
                sketch[layer, rows, :] = flipped[at : at + width]
    odd = section % 2 == 1
    first_out[...] = jnp.where(odd, kept[0], kept[-1]).astype(BF16)
    second_out[...] = jnp.where(odd, kept[-1], kept[0]).astype(BF16)


def finish(pos, messages, layers, tokens):
    rank = messages[0].shape[1]
    width = (messages[0].shape[0] - 8) // layers
    edge = jax.ShapeDtypeStruct((width, rank), BF16)
    return pl.pallas_call(
        functools.partial(finish_kernel, layers, len(messages), tokens),
        out_shape=(
            jax.ShapeDtypeStruct((layers, rank, width), F32),
            jax.ShapeDtypeStruct((layers, width, rank), F32),
            edge,
            edge,
        ),
        in_specs=[SMEM] + [VMEM] * len(messages),
        out_specs=(VMEM,) * 4,
        compiler_params=params(6),
        cost_estimate=cost(1e6, 2e6),
        name="finish",
    )(pos, *messages)


def products_kernel(layers, sections, pos, turned, one, two, out):
    section = pos[2]
    odd = section % 2 == 1
    one, two = one[...].astype(F32), two[...].astype(F32)
    rows = [turned[i] for i in range(layers)]
    before = jnp.where(section == 0, rows[0], jnp.where(odd, one, two))
    beyond = jnp.where(section == sections - 1, rows[-1], jnp.where(odd, two, one))
    pairs = [(before, before)] + [(row, row) for row in rows] + [(beyond, beyond)]
    chain = [before] + rows + [beyond]
    pairs += list(zip(chain[:-1], chain[1:]))
    out[...] = jnp.zeros_like(out)
    for n, (a, b) in enumerate(pairs):
        out[n : n + 1, :] = jnp.full((1, out.shape[1]), jnp.sum(a * b), F32)


def products(pos, turned, one, two, sections):
    layers = turned.shape[0]
    count = -(-(2 * layers + 3) // 8) * 8
    return pl.pallas_call(
        functools.partial(products_kernel, layers, sections),
        out_shape=jax.ShapeDtypeStruct((count, 128), F32),
        in_specs=[SMEM] + [VMEM] * 3,
        out_specs=VMEM,
        compiler_params=params(4),
        cost_estimate=cost(1e6, 1e6),
        name="products",
    )(pos, turned, one, two)


def ratios_kernel(layers, one, two, out):
    value = one[...] + two[...]
    squares = value[: layers + 2]
    chained = value[layers + 2 : 2 * layers + 3]
    ratio = chained / jnp.sqrt(squares[:-1] * squares[1:])
    out[:, 0:1] = ratio[:-1, 0:1]
    out[:, 1:2] = ratio[1:, 0:1]


def ratios(one, two, layers):
    return pl.pallas_call(
        functools.partial(ratios_kernel, layers),
        out_shape=jax.ShapeDtypeStruct((layers, 2), F32),
        in_specs=[VMEM] * 2,
        out_specs=VMEM,
        compiler_params=params(4),
        cost_estimate=cost(1e4, 1e4),
        name="ratios",
    )(one, two)


def local(activations, projection):
    layers, tok_rows, model = activations.shape
    block, rank = projection.shape
    groups, sections = lax.axis_size("tok"), lax.axis_size("section")
    chips, width = groups // 2, rank // groups
    tok, section = lax.axis_index("tok"), lax.axis_index("section")
    chip, core = tok // 2, tok % 2
    pos = jnp.stack([chip, core, section]).astype(jnp.int32)
    parts = min(sections, max(1, block // 128))
    deep = block // parts

    acts = activations.reshape(layers * tok_rows, model)
    mine_part, give_part = deal(pos, projection, width, deep)
    got_part = swap(give_part, "tok", 1)
    own = join(mine_part, got_part)

    fetched = {}
    for k in range(1, chips):
        low = k & -k
        fetched[k] = swap(own if k == low else fetched[k ^ low], "tok", 2 * low)

    mine, give = deal(pos, projection, width, block)
    got = swap(give, "tok", 1)

    order = sorted(fetched, key=lambda k: (bin(k).count("1"), -k))
    staged = {}
    for k in [0, order[-1]] + order[:-1]:
        staged[k] = stage(pos, acts, k, 2 * block)
        staged[k] = (staged[k], swap(staged[k], "tok", 1))

    far = {j: pick(pos, mine, got, parts, j) for j in range(1, parts) if j & (j - 1)}
    total = project(pos, [mine, got], parts, None, *staged[0], layers, False)
    for k in order:
        pieces = [fetched[k]]
        for j in range(1, parts):
            if k & (k - 1) == 0 and j & (j - 1):
                pieces.append(swap(far[j], "tok", 2 * k))
            else:
                pieces.append(swap(fetched[k], "section", j))
        total = project(pos, pieces, parts, total, *staged[k], layers, k == order[-1])
    split, sums = total

    messages = gram(pos, split, swap(split, "tok", 1), sums, swap(sums, "tok", 1), layers, chips)
    arrived = [messages[0]]
    for k in reversed(range(1, chips)):
        arrived.append(swap(messages[k], "tok", 2 * k))
    sketch, turned, first, second = finish(pos, arrived, layers, tok_rows * groups)

    first = swap(first, "section", 1)
    route = [(i, i + 1) for i in range(1, sections - 1, 2)]
    second = lax.ppermute(second, "section", route + [(b, a) for a, b in route])
    value = products(pos, turned, first, second, sections)
    mask = 1
    while 2 * mask < groups:
        value = value + swap(value, "tok", mask)
        mask *= 2
    return sketch, ratios(value, swap(value, "tok", mask), layers)


def solution(mesh):
    return jax.shard_map(
        local,
        mesh=mesh,
        in_specs=(P("section", "tok", None), P("tok", None)),
        out_specs=(P("section", None, "tok"), P("section", None)),
        check_vma=False,
    )
```

```python
import functools

import jax
import jax.numpy as jnp
from jax import lax
from jax.experimental import pallas as pl
from jax.experimental.pallas import tpu as pltpu
from jax.sharding import PartitionSpec as P


F32, BF16 = jnp.float32, jnp.bfloat16
VMEM = pl.BlockSpec(memory_space=pltpu.VMEM)
HBM = pl.BlockSpec(memory_space=pltpu.HBM)


def swap(block, axis, mask):
    return lax.ppermute(block, axis, [(i, i ^ mask) for i in range(lax.axis_size(axis))])


def params(mib):
    return pltpu.CompilerParams(vmem_limit_bytes=int(mib * 1024) << 10)


def place():
    tok = lax.axis_index("tok")
    return tok >> 1, tok & 1, lax.axis_index("section")


def cost(flops, moved):
    return pl.CostEstimate(flops=int(flops), bytes_accessed=int(moved), transcendentals=0)


def deal_kernel(width, rows, proj, mine, give, block, sem):
    _, core, section = place()
    start = 0
    if rows < proj.shape[0]:
        start = pl.multiple_of((section % (proj.shape[0] // rows)) * rows, 16)
    copy = pltpu.make_async_copy(proj.at[pl.ds(start, rows), :], block, sem)
    copy.start()
    rank, half = proj.shape[1], mine.shape[1]
    row = lax.broadcasted_iota(jnp.int32, (rank, half), 0)
    col = lax.broadcasted_iota(jnp.int32, (rank, half), 1)
    first = (col // width) * (2 * width) + col % width
    picks = [
        jnp.where(row == first + side * width, 1.0, 0.0).astype(BF16) for side in (core, 1 - core)
    ]
    copy.wait()
    for out, pick in zip((mine, give), picks):
        out[...] = jnp.dot(block[...], pick, preferred_element_type=F32).astype(BF16)


def deal(proj, width, rows):
    rank = proj.shape[1]
    half = jax.ShapeDtypeStruct((rows, rank // 2), BF16)
    return pl.pallas_call(
        functools.partial(deal_kernel, width, rows),
        out_shape=(half, half),
        in_specs=[HBM],
        out_specs=(VMEM, VMEM),
        scratch_shapes=[pltpu.VMEM((rows, rank), BF16), pltpu.SemaphoreType.DMA],
        compiler_params=params(4),
        cost_estimate=cost(2 * rows * rank * rank, 4 * rows * rank),
        name="deal",
    )(proj)


def stage_kernel(k, source, out, sem):
    deep = out.shape[1]
    columns = pl.ds(pl.multiple_of((place()[0] ^ k) * deep, 128), deep)
    copy = pltpu.make_async_copy(source.at[:, columns], out, sem)
    copy.start()
    copy.wait()


def stage(source, k, deep):
    rows = source.shape[0]
    return pl.pallas_call(
        functools.partial(stage_kernel, k),
        out_shape=jax.ShapeDtypeStruct((rows, deep), BF16),
        in_specs=[HBM],
        out_specs=VMEM,
        scratch_shapes=[pltpu.SemaphoreType.DMA],
        compiler_params=params(3),
        cost_estimate=cost(4e9, 4 * rows * deep),
        name="stage",
    )(source)


def join_kernel(upper, lower, out):
    deep = upper.shape[0]
    out[:deep, :] = upper[...]
    out[deep:, :] = lower[...]


def join(upper, lower):
    deep, half = upper.shape
    return pl.pallas_call(
        join_kernel,
        out_shape=jax.ShapeDtypeStruct((2 * deep, half), BF16),
        in_specs=[VMEM, VMEM],
        out_specs=VMEM,
        compiler_params=params(2),
        cost_estimate=cost(1e6, 8 * deep * half),
        name="join",
    )(upper, lower)


def pick_kernel(parts, j, upper, lower, out):
    deep = out.shape[0] // 2
    rows = pl.ds(pl.multiple_of(((place()[2] % parts) ^ j) * deep, 16), deep)
    out[:deep, :] = upper[rows, :]
    out[deep:, :] = lower[rows, :]


def pick(upper, lower, parts, j):
    rows, half = upper.shape
    return pl.pallas_call(
        functools.partial(pick_kernel, parts, j),
        out_shape=jax.ShapeDtypeStruct((2 * rows // parts, half), BF16),
        in_specs=[VMEM, VMEM],
        out_specs=VMEM,
        compiler_params=params(4),
        cost_estimate=cost(1e6, 8 * rows * half // parts),
        name="pick",
    )(upper, lower)


def project_kernel(keys, parts, started, last, layers, acts, other, *refs):
    pieces, refs = refs[: len(keys)], refs[len(keys) :]
    total = refs[0] if started else None
    outs = refs[started:]
    _, core, section = place()
    part = section % parts
    block = acts.shape[1] // 2
    offs = []
    for j, piece in zip(keys, pieces):
        if j is None:
            offs += [(core * block, block)] if not offs else [((1 - core) * block, block)]
        else:
            deep = block // parts
            offs += [(side * block + (part ^ j) * deep, deep) for side in (core, 1 - core)]
    offs = [pl.ds(pl.multiple_of(at, 128), deep) for at, deep in offs]
    weights = jnp.concatenate([piece[...] for piece in pieces], axis=0)
    rows = acts.shape[0] // layers
    kept = []
    for side, source in enumerate((acts, other)):
        for layer in range(layers):
            span = pl.ds(layer * rows, rows)
            left = jnp.concatenate([source[span, columns] for columns in offs], axis=1)
            value = jnp.dot(left, weights, preferred_element_type=F32)
            if started:
                value = value + total[side, span, :]
            if last:
                kept.append(value)
            else:
                outs[0][side, span, :] = value
    if not last:
        return
    split, sums = outs
    sums[...] = jnp.zeros_like(sums)
    for layer in range(layers):
        values = [kept[layer], kept[layers + layer]]
        column = jnp.sum(values[0] + values[1], axis=0, keepdims=True)
        sums[layer : layer + 1, :] = column
        mean = column / (2 * rows)
        for side in range(2):
            span = pl.ds(layer * rows, rows)
            value = values[side] - mean
            high = value.astype(BF16)
            split[0, side, span, :] = high
            split[1, side, span, :] = (value - high.astype(F32)).astype(BF16)


def project(pieces, keys, parts, total, acts, other, layers, last):
    rows, half = acts.shape[0], pieces[0].shape[1]
    deep = sum(piece.shape[0] for piece in pieces)
    if last:
        out_shape = (
            jax.ShapeDtypeStruct((2, 2, rows, half), BF16),
            jax.ShapeDtypeStruct((8, half), F32),
        )
        out_specs = (VMEM, VMEM)
    else:
        out_shape = jax.ShapeDtypeStruct((2, rows, half), F32)
        out_specs = VMEM
    started = [] if total is None else [total]
    return pl.pallas_call(
        functools.partial(project_kernel, keys, parts, len(started), last, layers),
        out_shape=out_shape,
        in_specs=[VMEM] * (2 + len(pieces) + len(started)),
        out_specs=out_specs,
        compiler_params=params(10),
        cost_estimate=cost(4 * rows * deep * half, 4 * rows * deep),
        name="project",
    )(acts, other, *pieces, *started)


def exponent(value):
    top = jnp.max(jnp.abs(value), axis=(0, 1), keepdims=True)
    return jnp.ceil(jnp.log2(jnp.maximum(top, 1e-30))) - 14.0


def gram_kernel(layers, chips, own, oth, own_sums, oth_sums, *outs):
    chip = place()[0]
    half = own.shape[3]
    rows = own.shape[2] // layers
    width = half // chips
    along_tokens = (((0,), (0,)), ((), ()))
    sums = jnp.concatenate([own_sums[...], oth_sums[...]], axis=1)
    tail = []
    for layer in range(layers):
        span = pl.ds(layer * rows, rows)
        left, right = [], []
        for part in range(2):
            here = jnp.concatenate([own[part, 0, span, :], own[part, 1, span, :]], axis=0)
            there = jnp.concatenate([oth[part, 1, span, :], oth[part, 0, span, :]], axis=0)
            left.append(here)
            right.append(jnp.concatenate([here, there], axis=1))
        gram = sum(
            lax.dot_general(left[i], right[j], along_tokens, preferred_element_type=F32)
            for i, j in ((0, 0), (0, 1), (1, 0))
        )
        power = exponent(gram)
        gram = gram * jnp.exp2(-power)
        blocks = [gram[i * width : (i + 1) * width] for i in range(chips)]
        for k, out in enumerate(outs):
            block = blocks[k]
            for i in range(1, chips):
                block = jnp.where(chip == i, blocks[i ^ k], block)
            out[layer * width : (layer + 1) * width, :] = block
        column = sums[layer : layer + 1]
        lift = exponent(column)
        column = column * jnp.exp2(-lift)
        high = column.astype(BF16).astype(F32)
        middle = (column - high).astype(BF16).astype(F32)
        line = jnp.zeros_like(column)
        tail += [high, middle, column - high - middle, line + power, line + lift]
    for out in outs:
        out[layers * width :, :] = jnp.zeros_like(out[layers * width :, :])
        for n, line in enumerate(tail):
            out[layers * width + n : layers * width + n + 1, :] = line


def tail_rows(layers):
    return -(-5 * layers // 16) * 16


def gram(own, oth, own_sums, oth_sums, layers, chips):
    rows, half = own.shape[2:]
    height = layers * (half // chips) + tail_rows(layers)
    message = jax.ShapeDtypeStruct((height, 2 * half), F32)
    return pl.pallas_call(
        functools.partial(gram_kernel, layers, chips),
        out_shape=(message,) * chips,
        in_specs=[VMEM] * 4,
        out_specs=(VMEM,) * chips,
        compiler_params=params(10),
        cost_estimate=cost(24 * rows * half * half, 16 * rows * half),
        name="gram",
    )(own, oth, own_sums, oth_sums)


def finish_kernel(layers, tokens, *refs):
    messages, (sketch, turned, first_out, second_out) = refs[:-4], refs[-4:]
    chips = len(messages)
    chip, core, section = place()
    rank = messages[0].shape[1]
    width = (messages[0].shape[0] - tail_rows(layers)) // layers
    half = rank // 2
    here = lax.broadcasted_iota(jnp.int32, (width, rank), 1)
    here = here == lax.broadcasted_iota(jnp.int32, (width, rank), 0) + chip * width
    kept = []
    for layer in range(layers):
        span = slice(layer * width, (layer + 1) * width)
        at = layers * width + 5 * layer
        value, sums = 0.0, []
        for message in messages:
            line = [message[at + n : at + n + 1, :] for n in range(5)]
            value = value + message[span, :] * jnp.exp2(line[3])
            sums.append((line[0] + line[1] + line[2]) * jnp.exp2(line[4]))
        mean = sum(sums) / tokens
        for total in sums:
            drift = total / (tokens // chips) - mean
            lifted = jnp.sum(jnp.where(here, drift, 0.0), axis=1, keepdims=True)
            value = value + (tokens // chips) * lifted * drift
        turned[layer] = value
        kept.append(value)
        flipped = value.T
        for i in range(chips):
            for side in range(2):
                at = side * half + i * width
                to = 2 * width * i + width * (core if side == 0 else 1 - core)
                rows = pl.ds(pl.multiple_of(to, 8), width)
                sketch[layer, rows, :] = flipped[at : at + width]
    odd = section % 2 == 1
    first_out[...] = jnp.where(odd, kept[0], kept[-1]).astype(BF16)
    second_out[...] = jnp.where(odd, kept[-1], kept[0]).astype(BF16)


def finish(messages, layers, tokens):
    height, rank = messages[0].shape
    width = (height - tail_rows(layers)) // layers
    edge = jax.ShapeDtypeStruct((width, rank), BF16)
    return pl.pallas_call(
        functools.partial(finish_kernel, layers, tokens),
        out_shape=(
            jax.ShapeDtypeStruct((layers, rank, width), F32),
            jax.ShapeDtypeStruct((layers, width, rank), F32),
            edge,
            edge,
        ),
        in_specs=[VMEM] * len(messages),
        out_specs=(VMEM,) * 4,
        compiler_params=params(6),
        cost_estimate=cost(1e6, 2e6),
        name="finish",
    )(*messages)


def products_kernel(layers, sections, turned, one, two, out):
    section = place()[2]
    odd = section % 2 == 1
    one, two = one[...].astype(F32), two[...].astype(F32)
    rows = [turned[i] for i in range(layers)]
    before = jnp.where(section == 0, rows[0], jnp.where(odd, one, two))
    beyond = jnp.where(section == sections - 1, rows[-1], jnp.where(odd, two, one))
    pairs = [(before, before)] + [(row, row) for row in rows] + [(beyond, beyond)]
    chain = [before] + rows + [beyond]
    pairs += list(zip(chain[:-1], chain[1:]))
    out[...] = jnp.zeros_like(out)
    for n, (a, b) in enumerate(pairs):
        out[n : n + 1, :] = jnp.full((1, out.shape[1]), jnp.sum(a * b), F32)


def products(turned, one, two, sections):
    layers = turned.shape[0]
    count = -(-(2 * layers + 3) // 8) * 8
    return pl.pallas_call(
        functools.partial(products_kernel, layers, sections),
        out_shape=jax.ShapeDtypeStruct((count, 128), F32),
        in_specs=[VMEM] * 3,
        out_specs=VMEM,
        compiler_params=params(4),
        cost_estimate=cost(1e6, 1e6),
        name="products",
    )(turned, one, two)


def ratios_kernel(layers, one, two, out):
    value = one[...] + two[...]
    squares = value[: layers + 2]
    chained = value[layers + 2 : 2 * layers + 3]
    ratio = chained / jnp.sqrt(squares[:-1] * squares[1:])
    out[:, 0:1] = ratio[:-1, 0:1]
    out[:, 1:2] = ratio[1:, 0:1]


def ratios(one, two, layers):
    return pl.pallas_call(
        functools.partial(ratios_kernel, layers),
        out_shape=jax.ShapeDtypeStruct((layers, 2), F32),
        in_specs=[VMEM] * 2,
        out_specs=VMEM,
        compiler_params=params(4),
        cost_estimate=cost(1e4, 1e4),
        name="ratios",
    )(one, two)


def local(activations, projection):
    layers, tok_rows, model = activations.shape
    block, rank = projection.shape
    groups, sections = lax.axis_size("tok"), lax.axis_size("section")
    chips, width = groups // 2, rank // groups
    parts = min(sections, max(1, block // 128))
    deep = block // parts

    acts = activations.reshape(layers * tok_rows, model)
    mine_part, give_part = deal(projection, width, deep)
    got_part = swap(give_part, "tok", 1)
    own = join(mine_part, got_part)

    fetched = {}
    for k in range(1, chips):
        low = k & -k
        fetched[k] = swap(own if k == low else fetched[k ^ low], "tok", 2 * low)

    mine, give = deal(projection, width, block)
    got = swap(give, "tok", 1)

    order = sorted(fetched, key=lambda k: (bin(k).count("1"), k))
    staged = {}
    for k in [0] + order:
        staged[k] = stage(acts, k, 2 * block)
        staged[k] = (staged[k], swap(staged[k], "tok", 1))

    far = {j: pick(mine, got, parts, j) for j in range(1, parts) if j & (j - 1)}
    pieces = {0: {}}
    for k in order:
        pieces[k] = {0: fetched[k]}
        for j in range(1, parts):
            if 1 < k == k & -k and j in far:
                pieces[k][j] = swap(far[j], "tok", 2 * k)
            else:
                pieces[k][j] = swap(fetched[k], "section", j)

    total = project([mine, got], (None, None), parts, None, *staged[0], layers, False)
    final, keys = order[-1], tuple(range(parts))
    steps = [(k, keys) for k in order[:-2]]
    steps += [(final, keys[:-1])] + [(k, keys) for k in order[-2:-1]] + [(final, keys[-1:])]
    steps = [step for step in steps if step[1]]
    for k, js in steps:
        last = (k, js) == steps[-1]
        chosen = [pieces[k][j] for j in js]
        total = project(chosen, js, parts, total, *staged[k], layers, last)
    split, sums = total

    messages = gram(split, swap(split, "tok", 1), sums, swap(sums, "tok", 1), layers, chips)
    arrived = [messages[0]]
    for k in reversed(range(1, chips)):
        arrived.append(swap(messages[k].astype(jnp.float16), "tok", 2 * k).astype(F32))
    sketch, turned, first, second = finish(arrived, layers, tok_rows * groups)

    first = swap(first, "section", 1)
    route = [(i, i + 1) for i in range(1, sections - 1, 2)]
    second = lax.ppermute(second, "section", route + [(b, a) for a, b in route])
    value = products(turned, first, second, sections)
    mask = 1
    while 2 * mask < groups:
        value = value + swap(value, "tok", mask)
        mask *= 2
    return sketch, ratios(value, swap(value, "tok", mask), layers)


def solution(mesh):
    return jax.shard_map(
        local,
        mesh=mesh,
        in_specs=(P("section", "tok", None), P("tok", None)),
        out_specs=(P("section", None, "tok"), P("section", None)),
        check_vma=False,
    )
```

```python
import functools

import jax
import jax.numpy as jnp
from jax import lax
from jax.experimental import pallas as pl
from jax.experimental.pallas import tpu as pltpu
from jax.sharding import PartitionSpec as P


F32, BF16 = jnp.float32, jnp.bfloat16
VMEM = pl.BlockSpec(memory_space=pltpu.VMEM)
HBM = pl.BlockSpec(memory_space=pltpu.HBM)


def swap(block, axis, mask):
    return lax.ppermute(block, axis, [(i, i ^ mask) for i in range(lax.axis_size(axis))])


def params(mib):
    return pltpu.CompilerParams(vmem_limit_bytes=int(mib * 1024) << 10)


def place():
    tok = lax.axis_index("tok")
    return tok >> 1, tok & 1, lax.axis_index("section")


def cost(flops, moved):
    return pl.CostEstimate(flops=int(flops), bytes_accessed=int(moved), transcendentals=0)


def deal_kernel(width, rows, proj, mine, give, block, sem):
    _, core, section = place()
    start = 0
    if rows < proj.shape[0]:
        start = pl.multiple_of((section % (proj.shape[0] // rows)) * rows, 16)
    copy = pltpu.make_async_copy(proj.at[pl.ds(start, rows), :], block, sem)
    copy.start()
    rank, half = proj.shape[1], mine.shape[1]
    row = lax.broadcasted_iota(jnp.int32, (rank, half), 0)
    col = lax.broadcasted_iota(jnp.int32, (rank, half), 1)
    first = (col // width) * (2 * width) + col % width
    picks = [
        jnp.where(row == first + side * width, 1.0, 0.0).astype(BF16) for side in (core, 1 - core)
    ]
    copy.wait()
    for out, pick in zip((mine, give), picks):
        out[...] = jnp.dot(block[...], pick, preferred_element_type=F32).astype(BF16)


def deal(proj, width, rows):
    rank = proj.shape[1]
    half = jax.ShapeDtypeStruct((rows, rank // 2), BF16)
    return pl.pallas_call(
        functools.partial(deal_kernel, width, rows),
        out_shape=(half, half),
        in_specs=[HBM],
        out_specs=(VMEM, VMEM),
        scratch_shapes=[pltpu.VMEM((rows, rank), BF16), pltpu.SemaphoreType.DMA],
        compiler_params=params(4),
        cost_estimate=cost(2 * rows * rank * rank, 4 * rows * rank),
        name="deal",
    )(proj)


def stage_kernel(k, source, out, sem):
    deep = out.shape[1]
    columns = pl.ds(pl.multiple_of((place()[0] ^ k) * deep, 128), deep)
    copy = pltpu.make_async_copy(source.at[:, columns], out, sem)
    copy.start()
    copy.wait()


def stage(source, k, deep):
    rows = source.shape[0]
    return pl.pallas_call(
        functools.partial(stage_kernel, k),
        out_shape=jax.ShapeDtypeStruct((rows, deep), BF16),
        in_specs=[HBM],
        out_specs=VMEM,
        scratch_shapes=[pltpu.SemaphoreType.DMA],
        compiler_params=params(3),
        cost_estimate=cost(4e9, 4 * rows * deep),
        name="stage",
    )(source)


def join_kernel(upper, lower, out):
    deep = upper.shape[0]
    out[:deep, :] = upper[...]
    out[deep:, :] = lower[...]


def join(upper, lower):
    deep, half = upper.shape
    return pl.pallas_call(
        join_kernel,
        out_shape=jax.ShapeDtypeStruct((2 * deep, half), BF16),
        in_specs=[VMEM, VMEM],
        out_specs=VMEM,
        compiler_params=params(2),
        cost_estimate=cost(1e6, 8 * deep * half),
        name="join",
    )(upper, lower)


def pick_kernel(parts, j, upper, lower, out):
    deep = out.shape[0] // 2
    rows = pl.ds(pl.multiple_of(((place()[2] % parts) ^ j) * deep, 16), deep)
    out[:deep, :] = upper[rows, :]
    out[deep:, :] = lower[rows, :]


def pick(upper, lower, parts, j):
    rows, half = upper.shape
    return pl.pallas_call(
        functools.partial(pick_kernel, parts, j),
        out_shape=jax.ShapeDtypeStruct((2 * rows // parts, half), BF16),
        in_specs=[VMEM, VMEM],
        out_specs=VMEM,
        compiler_params=params(4),
        cost_estimate=cost(1e6, 8 * rows * half // parts),
        name="pick",
    )(upper, lower)


def project_kernel(keys, parts, started, last, layers, acts, other, *refs):
    pieces, refs = refs[: len(keys)], refs[len(keys) :]
    total = refs[0] if started else None
    outs = refs[started:]
    _, core, section = place()
    part = section % parts
    block = acts.shape[1] // 2
    offs = []
    for j, piece in zip(keys, pieces):
        if j is None:
            offs += [(core * block, block)] if not offs else [((1 - core) * block, block)]
        else:
            deep = block // parts
            offs += [(side * block + (part ^ j) * deep, deep) for side in (core, 1 - core)]
    offs = [pl.ds(pl.multiple_of(at, 128), deep) for at, deep in offs]
    weights = jnp.concatenate([piece[...] for piece in pieces], axis=0)
    rows = acts.shape[0] // layers
    kept = []
    for side, source in enumerate((acts, other)):
        for layer in range(layers):
            span = pl.ds(layer * rows, rows)
            left = jnp.concatenate([source[span, columns] for columns in offs], axis=1)
            value = jnp.dot(left, weights, preferred_element_type=F32)
            if started:
                value = value + total[side, span, :]
            if last:
                kept.append(value)
            else:
                outs[0][side, span, :] = value
    if not last:
        return
    split, sums = outs
    sums[...] = jnp.zeros_like(sums)
    for layer in range(layers):
        values = [kept[layer], kept[layers + layer]]
        column = jnp.sum(values[0] + values[1], axis=0, keepdims=True)
        sums[layer : layer + 1, :] = column
        mean = column / (2 * rows)
        for side in range(2):
            span = pl.ds(layer * rows, rows)
            value = values[side] - mean
            high = value.astype(BF16)
            split[0, side, span, :] = high
            split[1, side, span, :] = (value - high.astype(F32)).astype(BF16)


def project(pieces, keys, parts, total, acts, other, layers, last):
    rows, half = acts.shape[0], pieces[0].shape[1]
    deep = sum(piece.shape[0] for piece in pieces)
    if last:
        out_shape = (
            jax.ShapeDtypeStruct((2, 2, rows, half), BF16),
            jax.ShapeDtypeStruct((8, half), F32),
        )
        out_specs = (VMEM, VMEM)
    else:
        out_shape = jax.ShapeDtypeStruct((2, rows, half), F32)
        out_specs = VMEM
    started = [] if total is None else [total]
    return pl.pallas_call(
        functools.partial(project_kernel, keys, parts, len(started), last, layers),
        out_shape=out_shape,
        in_specs=[VMEM] * (2 + len(pieces) + len(started)),
        out_specs=out_specs,
        compiler_params=params(10),
        cost_estimate=cost(4 * rows * deep * half, 4 * rows * deep),
        name="project",
    )(acts, other, *pieces, *started)


def exponent(value):
    top = jnp.max(jnp.abs(value), axis=(0, 1), keepdims=True)
    return jnp.ceil(jnp.log2(jnp.maximum(top, 1e-30))) - 14.0


def gram_kernel(layers, chips, own, oth, own_sums, oth_sums, *outs):
    chip = place()[0]
    half = own.shape[3]
    rows = own.shape[2] // layers
    width = half // chips
    along_tokens = (((0,), (0,)), ((), ()))
    sums = jnp.concatenate([own_sums[...], oth_sums[...]], axis=1)
    tail = []
    for layer in range(layers):
        span = pl.ds(layer * rows, rows)
        left, right = [], []
        for part in range(2):
            here = jnp.concatenate([own[part, 0, span, :], own[part, 1, span, :]], axis=0)
            there = jnp.concatenate([oth[part, 1, span, :], oth[part, 0, span, :]], axis=0)
            left.append(here)
            right.append(jnp.concatenate([here, there], axis=1))
        gram = sum(
            lax.dot_general(left[i], right[j], along_tokens, preferred_element_type=F32)
            for i, j in ((0, 0), (0, 1), (1, 0))
        )
        power = exponent(gram)
        gram = gram * jnp.exp2(-power)
        blocks = [gram[i * width : (i + 1) * width] for i in range(chips)]
        for k, out in enumerate(outs):
            block = blocks[k]
            for i in range(1, chips):
                block = jnp.where(chip == i, blocks[i ^ k], block)
            out[layer * width : (layer + 1) * width, :] = block
        column = sums[layer : layer + 1]
        lift = exponent(column)
        column = column * jnp.exp2(-lift)
        high = column.astype(BF16).astype(F32)
        middle = (column - high).astype(BF16).astype(F32)
        line = jnp.zeros_like(column)
        tail += [high, middle, column - high - middle, line + power, line + lift]
    for out in outs:
        out[layers * width :, :] = jnp.zeros_like(out[layers * width :, :])
        for n, line in enumerate(tail):
            out[layers * width + n : layers * width + n + 1, :] = line


def tail_rows(layers):
    return -(-5 * layers // 16) * 16


def gram(own, oth, own_sums, oth_sums, layers, chips):
    rows, half = own.shape[2:]
    height = layers * (half // chips) + tail_rows(layers)
    message = jax.ShapeDtypeStruct((height, 2 * half), F32)
    return pl.pallas_call(
        functools.partial(gram_kernel, layers, chips),
        out_shape=(message,) * chips,
        in_specs=[VMEM] * 4,
        out_specs=(VMEM,) * chips,
        compiler_params=params(10),
        cost_estimate=cost(24 * rows * half * half, 16 * rows * half),
        name="gram",
    )(own, oth, own_sums, oth_sums)


def finish_kernel(layers, tokens, *refs):
    messages, (sketch, turned, first_out, second_out) = refs[:-4], refs[-4:]
    chips = len(messages)
    chip, core, section = place()
    rank = messages[0].shape[1]
    width = (messages[0].shape[0] - tail_rows(layers)) // layers
    half = rank // 2
    here = lax.broadcasted_iota(jnp.int32, (width, rank), 1)
    here = here == lax.broadcasted_iota(jnp.int32, (width, rank), 0) + chip * width
    kept = []
    for layer in range(layers):
        span = slice(layer * width, (layer + 1) * width)
        at = layers * width + 5 * layer
        value, sums = 0.0, []
        for message in messages:
            line = [message[at + n : at + n + 1, :] for n in range(5)]
            value = value + message[span, :] * jnp.exp2(line[3])
            sums.append((line[0] + line[1] + line[2]) * jnp.exp2(line[4]))
        mean = sum(sums) / tokens
        for total in sums:
            drift = total / (tokens // chips) - mean
            lifted = jnp.sum(jnp.where(here, drift, 0.0), axis=1, keepdims=True)
            value = value + (tokens // chips) * lifted * drift
        turned[layer] = value
        kept.append(value)
        flipped = value.T
        for i in range(chips):
            for side in range(2):
                at = side * half + i * width
                to = 2 * width * i + width * (core if side == 0 else 1 - core)
                rows = pl.ds(pl.multiple_of(to, 8), width)
                sketch[layer, rows, :] = flipped[at : at + width]
    odd = section % 2 == 1
    first_out[...] = jnp.where(odd, kept[0], kept[-1]).astype(BF16)
    second_out[...] = jnp.where(odd, kept[-1], kept[0]).astype(BF16)


def finish(messages, layers, tokens):
    height, rank = messages[0].shape
    width = (height - tail_rows(layers)) // layers
    edge = jax.ShapeDtypeStruct((width, rank), BF16)
    return pl.pallas_call(
        functools.partial(finish_kernel, layers, tokens),
        out_shape=(
            jax.ShapeDtypeStruct((layers, rank, width), F32),
            jax.ShapeDtypeStruct((layers, width, rank), F32),
            edge,
            edge,
        ),
        in_specs=[VMEM] * len(messages),
        out_specs=(VMEM,) * 4,
        compiler_params=params(6),
        cost_estimate=cost(1e6, 2e6),
        name="finish",
    )(*messages)


def products_kernel(layers, sections, turned, one, two, out):
    section = place()[2]
    odd = section % 2 == 1
    one, two = one[...].astype(F32), two[...].astype(F32)
    rows = [turned[i] for i in range(layers)]
    before = jnp.where(section == 0, rows[0], jnp.where(odd, one, two))
    beyond = jnp.where(section == sections - 1, rows[-1], jnp.where(odd, two, one))
    pairs = [(before, before)] + [(row, row) for row in rows] + [(beyond, beyond)]
    chain = [before] + rows + [beyond]
    pairs += list(zip(chain[:-1], chain[1:]))
    out[...] = jnp.zeros_like(out)
    for n, (a, b) in enumerate(pairs):
        out[n : n + 1, :] = jnp.full((1, out.shape[1]), jnp.sum(a * b), F32)


def products(turned, one, two, sections):
    layers = turned.shape[0]
    count = -(-(2 * layers + 3) // 8) * 8
    return pl.pallas_call(
        functools.partial(products_kernel, layers, sections),
        out_shape=jax.ShapeDtypeStruct((count, 128), F32),
        in_specs=[VMEM] * 3,
        out_specs=VMEM,
        compiler_params=params(4),
        cost_estimate=cost(1e6, 1e6),
        name="products",
    )(turned, one, two)


def ratios_kernel(layers, one, two, out):
    value = one[...] + two[...]
    squares = value[: layers + 2]
    chained = value[layers + 2 : 2 * layers + 3]
    ratio = chained / jnp.sqrt(squares[:-1] * squares[1:])
    out[:, 0:1] = ratio[:-1, 0:1]
    out[:, 1:2] = ratio[1:, 0:1]


def ratios(one, two, layers):
    return pl.pallas_call(
        functools.partial(ratios_kernel, layers),
        out_shape=jax.ShapeDtypeStruct((layers, 2), F32),
        in_specs=[VMEM] * 2,
        out_specs=VMEM,
        compiler_params=params(4),
        cost_estimate=cost(1e4, 1e4),
        name="ratios",
    )(one, two)


def local(activations, projection):
    layers, tok_rows, model = activations.shape
    block, rank = projection.shape
    groups, sections = lax.axis_size("tok"), lax.axis_size("section")
    chips, width = groups // 2, rank // groups
    parts = min(sections, max(1, block // 128))
    deep = block // parts

    acts = activations.reshape(layers * tok_rows, model)
    mine_part, give_part = deal(projection, width, deep)
    got_part = swap(give_part, "tok", 1)
    own = join(mine_part, got_part)

    fetched = {}
    for k in range(1, chips):
        low = k & -k
        fetched[k] = swap(own if k == low else fetched[k ^ low], "tok", 2 * low)

    mine, give = deal(projection, width, block)
    got = swap(give, "tok", 1)

    order = sorted(fetched, key=lambda k: (bin(k).count("1"), k))
    staged = {}
    for k in [0] + order:
        staged[k] = stage(acts, k, 2 * block)
        staged[k] = (staged[k], swap(staged[k], "tok", 1))

    far = {j: pick(mine, got, parts, j) for j in range(1, parts) if j & (j - 1)}
    pieces = {0: {}}
    for k in order:
        pieces[k] = {0: fetched[k]}
        for j in range(1, parts):
            if k == 1 and j in far:
                pieces[k][j] = swap(far[j], "tok", 2 * k)
            else:
                pieces[k][j] = swap(fetched[k], "section", j)

    total = project([mine, got], (None, None), parts, None, *staged[0], layers, False)
    final, keys = order[-1], tuple(range(parts))
    steps = [(k, keys) for k in reversed(order[:-1])]
    steps += [(final, keys[: parts // 2]), (final, keys[parts // 2 :])]
    steps = [step for step in steps if step[1]]
    for k, js in steps:
        last = (k, js) == steps[-1]
        chosen = [pieces[k][j] for j in js]
        total = project(chosen, js, parts, total, *staged[k], layers, last)
    split, sums = total

    messages = gram(split, swap(split, "tok", 1), sums, swap(sums, "tok", 1), layers, chips)
    arrived = [messages[0]]
    for k in reversed(range(1, chips)):
        arrived.append(swap(messages[k].astype(jnp.float16), "tok", 2 * k).astype(F32))
    sketch, turned, first, second = finish(arrived, layers, tok_rows * groups)

    first = swap(first, "section", 1)
    route = [(i, i + 1) for i in range(1, sections - 1, 2)]
    second = lax.ppermute(second, "section", route + [(b, a) for a, b in route])
    value = products(turned, first, second, sections)
    mask = 1
    while 2 * mask < groups:
        value = value + swap(value, "tok", mask)
        mask *= 2
    return sketch, ratios(value, swap(value, "tok", mask), layers)


def solution(mesh):
    return jax.shard_map(
        local,
        mesh=mesh,
        in_specs=(P("section", "tok", None), P("tok", None)),
        out_specs=(P("section", None, "tok"), P("section", None)),
        check_vma=False,
    )
```

```python
import functools

import jax
import jax.numpy as jnp
from jax import lax
from jax.experimental import pallas as pl
from jax.experimental.pallas import tpu as pltpu
from jax.sharding import PartitionSpec as P


F32, BF16 = jnp.float32, jnp.bfloat16
VMEM = pl.BlockSpec(memory_space=pltpu.VMEM)
HBM = pl.BlockSpec(memory_space=pltpu.HBM)


def swap(block, axis, mask):
    return lax.ppermute(block, axis, [(i, i ^ mask) for i in range(lax.axis_size(axis))])


def params(mib):
    return pltpu.CompilerParams(vmem_limit_bytes=int(mib * 1024) << 10)


def place():
    tok = lax.axis_index("tok")
    return tok >> 1, tok & 1, lax.axis_index("section")


def cost(flops, moved):
    return pl.CostEstimate(flops=int(flops), bytes_accessed=int(moved), transcendentals=0)


def deal_kernel(width, rows, proj, mine, give, block, sem):
    _, core, section = place()
    start = 0
    if rows < proj.shape[0]:
        start = pl.multiple_of((section % (proj.shape[0] // rows)) * rows, 16)
    copy = pltpu.make_async_copy(proj.at[pl.ds(start, rows), :], block, sem)
    copy.start()
    rank, half = proj.shape[1], mine.shape[1]
    row = lax.broadcasted_iota(jnp.int32, (rank, half), 0)
    col = lax.broadcasted_iota(jnp.int32, (rank, half), 1)
    first = (col // width) * (2 * width) + col % width
    picks = [
        jnp.where(row == first + side * width, 1.0, 0.0).astype(BF16) for side in (core, 1 - core)
    ]
    copy.wait()
    for out, pick in zip((mine, give), picks):
        out[...] = jnp.dot(block[...], pick, preferred_element_type=F32).astype(BF16)


def deal(proj, width, rows):
    rank = proj.shape[1]
    half = jax.ShapeDtypeStruct((rows, rank // 2), BF16)
    return pl.pallas_call(
        functools.partial(deal_kernel, width, rows),
        out_shape=(half, half),
        in_specs=[HBM],
        out_specs=(VMEM, VMEM),
        scratch_shapes=[pltpu.VMEM((rows, rank), BF16), pltpu.SemaphoreType.DMA],
        compiler_params=params(4),
        cost_estimate=cost(2 * rows * rank * rank, 4 * rows * rank),
        name="deal",
    )(proj)


def stage_kernel(k, source, out, sem):
    deep = out.shape[1]
    columns = pl.ds(pl.multiple_of((place()[0] ^ k) * deep, 128), deep)
    copy = pltpu.make_async_copy(source.at[:, columns], out, sem)
    copy.start()
    copy.wait()


def stage(source, k, deep):
    rows = source.shape[0]
    return pl.pallas_call(
        functools.partial(stage_kernel, k),
        out_shape=jax.ShapeDtypeStruct((rows, deep), BF16),
        in_specs=[HBM],
        out_specs=VMEM,
        scratch_shapes=[pltpu.SemaphoreType.DMA],
        compiler_params=params(3),
        cost_estimate=cost(4e9, 4 * rows * deep),
        name="stage",
    )(source)


def join_kernel(upper, lower, out):
    deep = upper.shape[0]
    out[:deep, :] = upper[...]
    out[deep:, :] = lower[...]


def join(upper, lower):
    deep, half = upper.shape
    return pl.pallas_call(
        join_kernel,
        out_shape=jax.ShapeDtypeStruct((2 * deep, half), BF16),
        in_specs=[VMEM, VMEM],
        out_specs=VMEM,
        compiler_params=params(2),
        cost_estimate=cost(1e6, 8 * deep * half),
        name="join",
    )(upper, lower)


def pick_kernel(parts, j, upper, lower, out):
    deep = out.shape[0] // 2
    rows = pl.ds(pl.multiple_of(((place()[2] % parts) ^ j) * deep, 16), deep)
    out[:deep, :] = upper[rows, :]
    out[deep:, :] = lower[rows, :]


def pick(upper, lower, parts, j):
    rows, half = upper.shape
    return pl.pallas_call(
        functools.partial(pick_kernel, parts, j),
        out_shape=jax.ShapeDtypeStruct((2 * rows // parts, half), BF16),
        in_specs=[VMEM, VMEM],
        out_specs=VMEM,
        compiler_params=params(4),
        cost_estimate=cost(1e6, 8 * rows * half // parts),
        name="pick",
    )(upper, lower)


def project_kernel(keys, parts, started, last, layers, acts, other, *refs):
    pieces, refs = refs[: len(keys)], refs[len(keys) :]
    total = refs[0] if started else None
    outs = refs[started:]
    _, core, section = place()
    part = section % parts
    block = acts.shape[1] // 2
    offs = []
    for j, piece in zip(keys, pieces):
        if j is None:
            offs += [(core * block, block)] if not offs else [((1 - core) * block, block)]
        else:
            deep = block // parts
            offs += [(side * block + (part ^ j) * deep, deep) for side in (core, 1 - core)]
    offs = [pl.ds(pl.multiple_of(at, 128), deep) for at, deep in offs]
    weights = jnp.concatenate([piece[...] for piece in pieces], axis=0)
    rows = acts.shape[0] // layers
    kept = []
    for side, source in enumerate((acts, other)):
        for layer in range(layers):
            span = pl.ds(layer * rows, rows)
            left = jnp.concatenate([source[span, columns] for columns in offs], axis=1)
            value = jnp.dot(left, weights, preferred_element_type=F32)
            if started:
                value = value + total[side, span, :]
            if last:
                kept.append(value)
            else:
                outs[0][side, span, :] = value
    if not last:
        return
    split, sums = outs
    sums[...] = jnp.zeros_like(sums)
    for layer in range(layers):
        values = [kept[layer], kept[layers + layer]]
        column = jnp.sum(values[0] + values[1], axis=0, keepdims=True)
        sums[layer : layer + 1, :] = column
        mean = column / (2 * rows)
        for side in range(2):
            span = pl.ds(layer * rows, rows)
            value = values[side] - mean
            high = value.astype(BF16)
            split[0, side, span, :] = high
            split[1, side, span, :] = (value - high.astype(F32)).astype(BF16)


def project(pieces, keys, parts, total, acts, other, layers, last):
    rows, half = acts.shape[0], pieces[0].shape[1]
    deep = sum(piece.shape[0] for piece in pieces)
    if last:
        out_shape = (
            jax.ShapeDtypeStruct((2, 2, rows, half), BF16),
            jax.ShapeDtypeStruct((8, half), F32),
        )
        out_specs = (VMEM, VMEM)
    else:
        out_shape = jax.ShapeDtypeStruct((2, rows, half), F32)
        out_specs = VMEM
    started = [] if total is None else [total]
    return pl.pallas_call(
        functools.partial(project_kernel, keys, parts, len(started), last, layers),
        out_shape=out_shape,
        in_specs=[VMEM] * (2 + len(pieces) + len(started)),
        out_specs=out_specs,
        compiler_params=params(10),
        cost_estimate=cost(4 * rows * deep * half, 4 * rows * deep),
        name="project",
    )(acts, other, *pieces, *started)


def exponent(value):
    top = jnp.max(jnp.abs(value), axis=(0, 1), keepdims=True)
    return jnp.ceil(jnp.log2(jnp.maximum(top, 1e-30))) - 14.0


ALONG_TOKENS = (((0,), (0,)), ((), ()))


def halves(ref, layer, rows, swapped):
    span = pl.ds(layer * rows, rows)
    sides = (1, 0) if swapped else (0, 1)
    return [jnp.concatenate([ref[part, n, span, :] for n in sides], axis=0) for part in range(2)]


def outer(left, right):
    return sum(
        lax.dot_general(left[i], right[j], ALONG_TOKENS, preferred_element_type=F32)
        for i, j in ((0, 0), (0, 1), (1, 0))
    )


def inner_gram_kernel(layers, own, out):
    rows = own.shape[2] // layers
    for layer in range(layers):
        here = halves(own, layer, rows, False)
        out[layer] = outer(here, here)


def inner_gram(own, layers):
    rows, half = own.shape[2:]
    return pl.pallas_call(
        functools.partial(inner_gram_kernel, layers),
        out_shape=jax.ShapeDtypeStruct((layers, half, half), F32),
        in_specs=[VMEM],
        out_specs=VMEM,
        compiler_params=params(6),
        cost_estimate=cost(12 * rows * half * half, 16 * rows * half),
        name="inner_gram",
    )(own)


def gram_kernel(layers, chips, inner, own, oth, own_sums, oth_sums, *outs):
    chip = place()[0]
    half = own.shape[3]
    rows = own.shape[2] // layers
    width = half // chips
    sums = jnp.concatenate([own_sums[...], oth_sums[...]], axis=1)
    tail = []
    for layer in range(layers):
        cross = outer(halves(own, layer, rows, False), halves(oth, layer, rows, True))
        gram = jnp.concatenate([inner[layer], cross], axis=1)
        power = exponent(gram)
        gram = gram * jnp.exp2(-power)
        blocks = [gram[i * width : (i + 1) * width] for i in range(chips)]
        for k, out in enumerate(outs):
            block = blocks[k]
            for i in range(1, chips):
                block = jnp.where(chip == i, blocks[i ^ k], block)
            out[layer * width : (layer + 1) * width, :] = block
        column = sums[layer : layer + 1]
        lift = exponent(column)
        column = column * jnp.exp2(-lift)
        high = column.astype(BF16).astype(F32)
        middle = (column - high).astype(BF16).astype(F32)
        line = jnp.zeros((1, half), F32)
        powers = jnp.concatenate([line + power, line + lift], axis=1)
        tail += [high, middle, column - high - middle, powers]
    for out in outs:
        if len(tail) < tail_rows(layers):
            out[layers * width :, :] = jnp.zeros_like(out[layers * width :, :])
        for n, line in enumerate(tail):
            out[layers * width + n : layers * width + n + 1, :] = line


def tail_rows(layers):
    return -(-4 * layers // 8) * 8


def gram(inner, own, oth, own_sums, oth_sums, layers, chips):
    rows, half = own.shape[2:]
    height = layers * (half // chips) + tail_rows(layers)
    message = jax.ShapeDtypeStruct((height, 2 * half), F32)
    return pl.pallas_call(
        functools.partial(gram_kernel, layers, chips),
        out_shape=(message,) * chips,
        in_specs=[VMEM] * 5,
        out_specs=(VMEM,) * chips,
        compiler_params=params(10),
        cost_estimate=cost(12 * rows * half * half, 16 * rows * half),
        name="gram",
    )(inner, own, oth, own_sums, oth_sums)


def finish_kernel(layers, tokens, *refs):
    messages, (sketch, turned, first_out, second_out) = refs[:-4], refs[-4:]
    chips = len(messages)
    chip, core, section = place()
    rank = messages[0].shape[1]
    width = (messages[0].shape[0] - tail_rows(layers)) // layers
    half = rank // 2
    here = lax.broadcasted_iota(jnp.int32, (width, rank), 1)
    here = here == lax.broadcasted_iota(jnp.int32, (width, rank), 0) + chip * width
    kept = []
    for layer in range(layers):
        span = slice(layer * width, (layer + 1) * width)
        at = layers * width + 4 * layer
        value, sums = 0.0, []
        for message in messages:
            line = [message[at + n : at + n + 1, :] for n in range(4)]
            scale = jnp.exp2(line[3])
            value = value + message[span, :] * scale[:, :1]
            sums.append((line[0] + line[1] + line[2]) * scale[:, rank - 1 :])
        mean = sum(sums) / tokens
        for total in sums:
            drift = total / (tokens // chips) - mean
            lifted = jnp.sum(jnp.where(here, drift, 0.0), axis=1, keepdims=True)
            value = value + (tokens // chips) * lifted * drift
        turned[layer] = value
        kept.append(value)
        flipped = value.T
        for i in range(chips):
            for side in range(2):
                at = side * half + i * width
                to = 2 * width * i + width * (core if side == 0 else 1 - core)
                rows = pl.ds(pl.multiple_of(to, 8), width)
                sketch[layer, rows, :] = flipped[at : at + width]
    odd = section % 2 == 1
    first_out[...] = jnp.where(odd, kept[0], kept[-1]).astype(BF16)
    second_out[...] = jnp.where(odd, kept[-1], kept[0]).astype(BF16)


def finish(messages, layers, tokens):
    height, rank = messages[0].shape
    width = (height - tail_rows(layers)) // layers
    edge = jax.ShapeDtypeStruct((width, rank), BF16)
    return pl.pallas_call(
        functools.partial(finish_kernel, layers, tokens),
        out_shape=(
            jax.ShapeDtypeStruct((layers, rank, width), F32),
            jax.ShapeDtypeStruct((layers, width, rank), F32),
            edge,
            edge,
        ),
        in_specs=[VMEM] * len(messages),
        out_specs=(VMEM,) * 4,
        compiler_params=params(6),
        cost_estimate=cost(1e6, 2e6),
        name="finish",
    )(*messages)


def products_kernel(layers, sections, turned, one, two, out):
    section = place()[2]
    odd = section % 2 == 1
    one, two = one[...].astype(F32), two[...].astype(F32)
    rows = [turned[i] for i in range(layers)]
    before = jnp.where(section == 0, rows[0], jnp.where(odd, one, two))
    beyond = jnp.where(section == sections - 1, rows[-1], jnp.where(odd, two, one))
    pairs = [(before, before)] + [(row, row) for row in rows] + [(beyond, beyond)]
    chain = [before] + rows + [beyond]
    pairs += list(zip(chain[:-1], chain[1:]))
    out[...] = jnp.zeros_like(out)
    for n, (a, b) in enumerate(pairs):
        out[n : n + 1, :] = jnp.full((1, out.shape[1]), jnp.sum(a * b), F32)


def products(turned, one, two, sections):
    layers = turned.shape[0]
    count = -(-(2 * layers + 3) // 8) * 8
    return pl.pallas_call(
        functools.partial(products_kernel, layers, sections),
        out_shape=jax.ShapeDtypeStruct((count, 128), F32),
        in_specs=[VMEM] * 3,
        out_specs=VMEM,
        compiler_params=params(4),
        cost_estimate=cost(1e6, 1e6),
        name="products",
    )(turned, one, two)


def ratios_kernel(layers, one, two, out):
    value = one[...] + two[...]
    squares = value[: layers + 2]
    chained = value[layers + 2 : 2 * layers + 3]
    ratio = chained / jnp.sqrt(squares[:-1] * squares[1:])
    out[:, 0:1] = ratio[:-1, 0:1]
    out[:, 1:2] = ratio[1:, 0:1]


def ratios(one, two, layers):
    return pl.pallas_call(
        functools.partial(ratios_kernel, layers),
        out_shape=jax.ShapeDtypeStruct((layers, 2), F32),
        in_specs=[VMEM] * 2,
        out_specs=VMEM,
        compiler_params=params(4),
        cost_estimate=cost(1e4, 1e4),
        name="ratios",
    )(one, two)


def local(activations, projection):
    layers, tok_rows, model = activations.shape
    block, rank = projection.shape
    groups, sections = lax.axis_size("tok"), lax.axis_size("section")
    chips, width = groups // 2, rank // groups
    parts = min(sections, max(1, block // 128))
    deep = block // parts

    acts = activations.reshape(layers * tok_rows, model)
    mine_part, give_part = deal(projection, width, deep)
    got_part = swap(give_part, "tok", 1)
    own = join(mine_part, got_part)

    fetched = {}
    for k in range(1, chips):
        low = k & -k
        fetched[k] = swap(own if k == low else fetched[k ^ low], "tok", 2 * low)

    mine, give = deal(projection, width, block)
    got = swap(give, "tok", 1)

    order = sorted(fetched, key=lambda k: (bin(k).count("1"), k))
    staged = {}
    for k in [0] + order:
        staged[k] = stage(acts, k, 2 * block)
        staged[k] = (staged[k], swap(staged[k], "tok", 1))

    far = {j: pick(mine, got, parts, j) for j in range(1, parts) if j & (j - 1)}
    pieces = {0: {}}
    for k in order:
        pieces[k] = {0: fetched[k]}
        for j in range(1, parts):
            if j in far and k in (1, order[-1]):
                pieces[k][j] = swap(far[j], "tok", 2 * k)
            else:
                pieces[k][j] = swap(fetched[k], "section", j)

    total = project([mine, got], (None, None), parts, None, *staged[0], layers, False)
    final, keys = order[-1], tuple(range(parts))
    late = tuple(j for j in keys[1:] if j not in far)
    steps = [(k, keys) for k in reversed(order[:-1])]
    steps += [(final, tuple(j for j in keys if j not in late)), (final, late)]
    steps = [step for step in steps if step[1]]
    for k, js in steps:
        last = (k, js) == steps[-1]
        chosen = [pieces[k][j] for j in js]
        total = project(chosen, js, parts, total, *staged[k], layers, last)
    split, sums = total

    split_oth = swap(split, "tok", 1)
    sums_oth = swap(sums, "tok", 1)
    inner = inner_gram(split, layers)
    messages = gram(inner, split, split_oth, sums, sums_oth, layers, chips)
    arrived = [messages[0]]
    for k in reversed(range(1, chips)):
        arrived.append(swap(messages[k].astype(jnp.float16), "tok", 2 * k).astype(F32))
    sketch, turned, first, second = finish(arrived, layers, tok_rows * groups)

    route = [(i, i + 1) for i in range(1, sections - 1, 2)]
    second = lax.ppermute(second, "section", route + [(b, a) for a, b in route])
    first = swap(first, "section", 1)
    value = products(turned, first, second, sections)
    mask = 1
    while 2 * mask < groups:
        value = value + swap(value, "tok", mask)
        mask *= 2
    return sketch, ratios(value, swap(value, "tok", mask), layers)


def solution(mesh):
    return jax.shard_map(
        local,
        mesh=mesh,
        in_specs=(P("section", "tok", None), P("tok", None)),
        out_specs=(P("section", None, "tok"), P("section", None)),
        check_vma=False,
    )
```

```python
import functools

import jax
import jax.numpy as jnp
from jax import lax
from jax.experimental import pallas as pl
from jax.experimental.pallas import tpu as pltpu
from jax.sharding import PartitionSpec as P


F32, BF16 = jnp.float32, jnp.bfloat16
VMEM = pl.BlockSpec(memory_space=pltpu.VMEM)
HBM = pl.BlockSpec(memory_space=pltpu.HBM)


def swap(block, axis, mask):
    return lax.ppermute(block, axis, [(i, i ^ mask) for i in range(lax.axis_size(axis))])


def params(mib):
    return pltpu.CompilerParams(vmem_limit_bytes=int(mib * 1024) << 10)


def place():
    tok = lax.axis_index("tok")
    return tok >> 1, tok & 1, lax.axis_index("section")


def cost(flops, moved):
    return pl.CostEstimate(flops=int(flops), bytes_accessed=int(moved), transcendentals=0)


def deal_kernel(width, proj, mine, give):
    core = place()[1]
    rank, half = proj.shape[1], mine.shape[1]
    row = lax.broadcasted_iota(jnp.int32, (rank, half), 0)
    col = lax.broadcasted_iota(jnp.int32, (rank, half), 1)
    first = (col // width) * (2 * width) + col % width
    picks = [
        jnp.where(row == first + side * width, 1.0, 0.0).astype(BF16) for side in (core, 1 - core)
    ]
    for out, pick in zip((mine, give), picks):
        out[...] = jnp.dot(proj[...], pick, preferred_element_type=F32).astype(BF16)


def deal(proj, width):
    rows, rank = proj.shape
    half = jax.ShapeDtypeStruct((rows, rank // 2), BF16)
    return pl.pallas_call(
        functools.partial(deal_kernel, width),
        out_shape=(half, half),
        in_specs=[VMEM],
        out_specs=(VMEM, VMEM),
        compiler_params=params(4),
        cost_estimate=cost(2 * rows * rank * rank, 4 * rows * rank),
        name="deal",
    )(proj)


def stage_kernel(k, source, out, sem):
    deep = out.shape[1]
    columns = pl.ds(pl.multiple_of((place()[0] ^ k) * deep, 128), deep)
    copy = pltpu.make_async_copy(source.at[:, columns], out, sem)
    copy.start()
    copy.wait()


def stage(source, k, deep):
    rows = source.shape[0]
    return pl.pallas_call(
        functools.partial(stage_kernel, k),
        out_shape=jax.ShapeDtypeStruct((rows, deep), BF16),
        in_specs=[HBM],
        out_specs=VMEM,
        scratch_shapes=[pltpu.SemaphoreType.DMA],
        compiler_params=params(3),
        cost_estimate=cost(4e9, 4 * rows * deep),
        name="stage",
    )(source)


def join_kernel(upper, lower, out):
    deep = upper.shape[0]
    out[:deep, :] = upper[...]
    out[deep:, :] = lower[...]


def join(upper, lower):
    deep, half = upper.shape
    return pl.pallas_call(
        join_kernel,
        out_shape=jax.ShapeDtypeStruct((2 * deep, half), BF16),
        in_specs=[VMEM, VMEM],
        out_specs=VMEM,
        compiler_params=params(2),
        cost_estimate=cost(1e6, 8 * deep * half),
        name="join",
    )(upper, lower)


def pick_kernel(parts, j, upper, lower, out):
    deep = out.shape[0] // 2
    rows = pl.ds(pl.multiple_of(((place()[2] % parts) ^ j) * deep, 16), deep)
    out[:deep, :] = upper[rows, :]
    out[deep:, :] = lower[rows, :]


def pick(upper, lower, parts, j):
    rows, half = upper.shape
    return pl.pallas_call(
        functools.partial(pick_kernel, parts, j),
        out_shape=jax.ShapeDtypeStruct((2 * rows // parts, half), BF16),
        in_specs=[VMEM, VMEM],
        out_specs=VMEM,
        compiler_params=params(4),
        cost_estimate=cost(1e6, 8 * rows * half // parts),
        name="pick",
    )(upper, lower)


def project_kernel(keys, parts, started, last, layers, acts, other, *refs):
    pieces, refs = refs[: len(keys)], refs[len(keys) :]
    total = refs[0] if started else None
    outs = refs[started:]
    _, core, section = place()
    part = section % parts
    block = acts.shape[1] // 2
    offs = []
    for j, piece in zip(keys, pieces):
        if j is None:
            offs += [(core * block, block)] if not offs else [((1 - core) * block, block)]
        else:
            deep = block // parts
            offs += [(side * block + (part ^ j) * deep, deep) for side in (core, 1 - core)]
    offs = [pl.ds(pl.multiple_of(at, 128), deep) for at, deep in offs]
    weights = jnp.concatenate([piece[...] for piece in pieces], axis=0)
    rows = acts.shape[0] // layers
    kept = []
    for side, source in enumerate((acts, other)):
        for layer in range(layers):
            span = pl.ds(layer * rows, rows)
            left = jnp.concatenate([source[span, columns] for columns in offs], axis=1)
            value = jnp.dot(left, weights, preferred_element_type=F32)
            if started:
                value = value + total[side, span, :]
            if last:
                kept.append(value)
            else:
                outs[0][side, span, :] = value
    if not last:
        return
    split, sums = outs
    sums[...] = jnp.zeros_like(sums)
    for layer in range(layers):
        values = [kept[layer], kept[layers + layer]]
        column = jnp.sum(values[0] + values[1], axis=0, keepdims=True)
        sums[layer : layer + 1, :] = column
        mean = column / (2 * rows)
        for side in range(2):
            span = pl.ds(layer * rows, rows)
            value = values[side] - mean
            high = value.astype(BF16)
            split[0, side, span, :] = high
            split[1, side, span, :] = (value - high.astype(F32)).astype(BF16)


def project(pieces, keys, parts, total, acts, other, layers, last):
    rows, half = acts.shape[0], pieces[0].shape[1]
    deep = sum(piece.shape[0] for piece in pieces)
    if last:
        out_shape = (
            jax.ShapeDtypeStruct((2, 2, rows, half), BF16),
            jax.ShapeDtypeStruct((8, half), F32),
        )
        out_specs = (VMEM, VMEM)
    else:
        out_shape = jax.ShapeDtypeStruct((2, rows, half), F32)
        out_specs = VMEM
    started = [] if total is None else [total]
    return pl.pallas_call(
        functools.partial(project_kernel, keys, parts, len(started), last, layers),
        out_shape=out_shape,
        in_specs=[VMEM] * (2 + len(pieces) + len(started)),
        out_specs=out_specs,
        compiler_params=params(10),
        cost_estimate=cost(4 * rows * deep * half, 4 * rows * deep),
        name="project",
    )(acts, other, *pieces, *started)


def exponent(value):
    top = jnp.max(jnp.abs(value), axis=(0, 1), keepdims=True)
    return jnp.ceil(jnp.log2(jnp.maximum(top, 1e-30))) - 14.0


ALONG_TOKENS = (((0,), (0,)), ((), ()))


def halves(ref, layer, rows, swapped):
    span = pl.ds(layer * rows, rows)
    sides = (1, 0) if swapped else (0, 1)
    return [jnp.concatenate([ref[part, n, span, :] for n in sides], axis=0) for part in range(2)]


def outer(left, right):
    return sum(
        lax.dot_general(left[i], right[j], ALONG_TOKENS, preferred_element_type=F32)
        for i, j in ((0, 0), (0, 1), (1, 0))
    )


def inner_gram_kernel(layers, own, out):
    rows = own.shape[2] // layers
    for layer in range(layers):
        here = halves(own, layer, rows, False)
        out[layer] = outer(here, here)


def inner_gram(own, layers):
    rows, half = own.shape[2:]
    return pl.pallas_call(
        functools.partial(inner_gram_kernel, layers),
        out_shape=jax.ShapeDtypeStruct((layers, half, half), F32),
        in_specs=[VMEM],
        out_specs=VMEM,
        compiler_params=params(6),
        cost_estimate=cost(12 * rows * half * half, 16 * rows * half),
        name="inner_gram",
    )(own)


def gram_kernel(layers, chips, inner, own, oth, own_sums, oth_sums, *outs):
    chip = place()[0]
    half = own.shape[3]
    rows = own.shape[2] // layers
    width = half // chips
    sums = jnp.concatenate([own_sums[...], oth_sums[...]], axis=1)
    tail = []
    for layer in range(layers):
        cross = outer(halves(own, layer, rows, False), halves(oth, layer, rows, True))
        gram = jnp.concatenate([inner[layer], cross], axis=1)
        power = exponent(gram)
        gram = gram * jnp.exp2(-power)
        blocks = [gram[i * width : (i + 1) * width] for i in range(chips)]
        for k, out in enumerate(outs):
            block = blocks[k]
            for i in range(1, chips):
                block = jnp.where(chip == i, blocks[i ^ k], block)
            out[layer * width : (layer + 1) * width, :] = block
        column = sums[layer : layer + 1]
        lift = exponent(column)
        column = column * jnp.exp2(-lift)
        high = column.astype(BF16).astype(F32)
        middle = (column - high).astype(BF16).astype(F32)
        line = jnp.zeros((1, half), F32)
        powers = jnp.concatenate([line + power, line + lift], axis=1)
        tail += [high, middle, column - high - middle, powers]
    for out in outs:
        if len(tail) < tail_rows(layers):
            out[layers * width :, :] = jnp.zeros_like(out[layers * width :, :])
        for n, line in enumerate(tail):
            out[layers * width + n : layers * width + n + 1, :] = line


def tail_rows(layers):
    return -(-4 * layers // 8) * 8


def gram(inner, own, oth, own_sums, oth_sums, layers, chips):
    rows, half = own.shape[2:]
    height = layers * (half // chips) + tail_rows(layers)
    message = jax.ShapeDtypeStruct((height, 2 * half), F32)
    return pl.pallas_call(
        functools.partial(gram_kernel, layers, chips),
        out_shape=(message,) * chips,
        in_specs=[VMEM] * 5,
        out_specs=(VMEM,) * chips,
        compiler_params=params(10),
        cost_estimate=cost(12 * rows * half * half, 16 * rows * half),
        name="gram",
    )(inner, own, oth, own_sums, oth_sums)


def finish_kernel(layers, tokens, *refs):
    messages, (sketch, turned, first_out, second_out) = refs[:-4], refs[-4:]
    chips = len(messages)
    chip, core, section = place()
    rank = messages[0].shape[1]
    width = (messages[0].shape[0] - tail_rows(layers)) // layers
    half = rank // 2
    here = lax.broadcasted_iota(jnp.int32, (width, rank), 1)
    here = here == lax.broadcasted_iota(jnp.int32, (width, rank), 0) + chip * width
    kept = []
    for layer in range(layers):
        span = slice(layer * width, (layer + 1) * width)
        at = layers * width + 4 * layer
        value, sums = 0.0, []
        for message in messages:
            line = [message[at + n : at + n + 1, :] for n in range(4)]
            scale = jnp.exp2(line[3])
            value = value + message[span, :] * scale[:, :1]
            sums.append((line[0] + line[1] + line[2]) * scale[:, rank - 1 :])
        mean = sum(sums) / tokens
        for total in sums:
            drift = total / (tokens // chips) - mean
            lifted = jnp.sum(jnp.where(here, drift, 0.0), axis=1, keepdims=True)
            value = value + (tokens // chips) * lifted * drift
        turned[layer] = value
        kept.append(value)
        flipped = value.T
        for i in range(chips):
            for side in range(2):
                at = side * half + i * width
                to = 2 * width * i + width * (core if side == 0 else 1 - core)
                rows = pl.ds(pl.multiple_of(to, 8), width)
                sketch[layer, rows, :] = flipped[at : at + width]
    odd = section % 2 == 1
    first_out[...] = jnp.where(odd, kept[0], kept[-1]).astype(BF16)
    second_out[...] = jnp.where(odd, kept[-1], kept[0]).astype(BF16)


def finish(messages, layers, tokens):
    height, rank = messages[0].shape
    width = (height - tail_rows(layers)) // layers
    edge = jax.ShapeDtypeStruct((width, rank), BF16)
    return pl.pallas_call(
        functools.partial(finish_kernel, layers, tokens),
        out_shape=(
            jax.ShapeDtypeStruct((layers, rank, width), F32),
            jax.ShapeDtypeStruct((layers, width, rank), F32),
            edge,
            edge,
        ),
        in_specs=[VMEM] * len(messages),
        out_specs=(VMEM,) * 4,
        compiler_params=params(6),
        cost_estimate=cost(1e6, 2e6),
        name="finish",
    )(*messages)


def products_kernel(layers, sections, turned, one, two, out):
    section = place()[2]
    odd = section % 2 == 1
    one, two = one[...].astype(F32), two[...].astype(F32)
    rows = [turned[i] for i in range(layers)]
    before = jnp.where(section == 0, rows[0], jnp.where(odd, one, two))
    beyond = jnp.where(section == sections - 1, rows[-1], jnp.where(odd, two, one))
    pairs = [(before, before)] + [(row, row) for row in rows] + [(beyond, beyond)]
    chain = [before] + rows + [beyond]
    pairs += list(zip(chain[:-1], chain[1:]))
    out[...] = jnp.zeros_like(out)
    for n, (a, b) in enumerate(pairs):
        out[n : n + 1, :] = jnp.full((1, out.shape[1]), jnp.sum(a * b), F32)


def products(turned, one, two, sections):
    layers = turned.shape[0]
    count = -(-(2 * layers + 3) // 8) * 8
    return pl.pallas_call(
        functools.partial(products_kernel, layers, sections),
        out_shape=jax.ShapeDtypeStruct((count, 128), F32),
        in_specs=[VMEM] * 3,
        out_specs=VMEM,
        compiler_params=params(4),
        cost_estimate=cost(1e6, 1e6),
        name="products",
    )(turned, one, two)


def ratios_kernel(layers, *refs):
    out = refs[-1]
    value = sum(ref[...] for ref in refs[:-1])
    squares = value[: layers + 2]
    chained = value[layers + 2 : 2 * layers + 3]
    ratio = chained / jnp.sqrt(squares[:-1] * squares[1:])
    out[:, 0:1] = ratio[:-1, 0:1]
    out[:, 1:2] = ratio[1:, 0:1]


def ratios(shares, layers):
    return pl.pallas_call(
        functools.partial(ratios_kernel, layers),
        out_shape=jax.ShapeDtypeStruct((layers, 2), F32),
        in_specs=[VMEM] * len(shares),
        out_specs=VMEM,
        compiler_params=params(4),
        cost_estimate=cost(1e4, 1e4),
        name="ratios",
    )(*shares)


def local(activations, projection):
    layers, tok_rows, model = activations.shape
    block, rank = projection.shape
    groups, sections = lax.axis_size("tok"), lax.axis_size("section")
    chips, width = groups // 2, rank // groups
    parts = min(sections, max(1, block // 128))
    deep = block // parts

    acts = activations.reshape(layers * tok_rows, model)
    start = (lax.axis_index("section") & (parts - 1)) * deep
    part = lax.dynamic_slice_in_dim(projection, start, deep, 0)
    mine_part, give_part = deal(part, width)
    got_part = swap(give_part, "tok", 1)
    own = join(mine_part, got_part)

    fetched = {}
    for k in range(1, chips):
        low = k & -k
        fetched[k] = swap(own if k == low else fetched[k ^ low], "tok", 2 * low)

    mine, give = deal(projection, width)
    got = swap(give, "tok", 1)

    order = sorted(fetched, key=lambda k: (bin(k).count("1"), k))
    staged = {}
    for k in [0] + order:
        staged[k] = stage(acts, k, 2 * block)
        staged[k] = (staged[k], swap(staged[k], "tok", 1))

    far = {j: pick(mine, got, parts, j) for j in range(1, parts) if j & (j - 1)}
    pieces = {0: {}}
    for k in order:
        pieces[k] = {0: fetched[k]}
        for j in range(1, parts):
            if j in far and k in (1, order[-1]):
                pieces[k][j] = swap(far[j], "tok", 2 * k)
            else:
                pieces[k][j] = swap(fetched[k], "section", j)

    total = project([mine, got], (None, None), parts, None, *staged[0], layers, False)
    final, keys = order[-1], tuple(range(parts))
    late = tuple(j for j in keys[1:] if j not in far)
    steps = [(k, keys) for k in reversed(order[1:-1])]
    steps += [(final, tuple(j for j in keys if j not in late))]
    steps += [(k, keys) for k in order[:-1][:1]] + [(final, late)]
    steps = [step for step in steps if step[1]]
    for k, js in steps:
        last = (k, js) == steps[-1]
        chosen = [pieces[k][j] for j in js]
        total = project(chosen, js, parts, total, *staged[k], layers, last)
    split, sums = total

    split_oth = swap(split, "tok", 1)
    sums_oth = swap(sums, "tok", 1)
    inner = inner_gram(split, layers)
    messages = gram(inner, split, split_oth, sums, sums_oth, layers, chips)
    arrived = [messages[0]]
    for k in reversed(range(1, chips)):
        arrived.append(swap(messages[k].astype(jnp.float16), "tok", 2 * k).astype(F32))
    sketch, turned, first, second = finish(arrived, layers, tok_rows * groups)

    route = [(i, i + 1) for i in range(1, sections - 1, 2)]
    second = lax.ppermute(second, "section", route + [(b, a) for a, b in route])
    first = swap(first, "section", 1)
    value = products(turned, first, second, sections)
    value = value + swap(value, "tok", 1)
    if chips <= 4:
        others = []
        for k in reversed(range(1, chips)):
            others.append(swap(value, "tok", 2 * k))
    else:
        mask = 2
        while 2 * mask < groups:
            value = value + swap(value, "tok", mask)
            mask *= 2
        others = [swap(value, "tok", mask)]
    return sketch, ratios([value] + others, layers)


def solution(mesh):
    return jax.shard_map(
        local,
        mesh=mesh,
        in_specs=(P("section", "tok", None), P("tok", None)),
        out_specs=(P("section", None, "tok"), P("section", None)),
        check_vma=False,
    )
```

```python
import functools

import jax
import jax.numpy as jnp
from jax import lax
from jax.experimental import pallas as pl
from jax.experimental.pallas import tpu as pltpu
from jax.sharding import PartitionSpec as P


F32, BF16 = jnp.float32, jnp.bfloat16
VMEM = pl.BlockSpec(memory_space=pltpu.VMEM)
HBM = pl.BlockSpec(memory_space=pltpu.HBM)


def swap(block, axis, mask):
    return lax.ppermute(block, axis, [(i, i ^ mask) for i in range(lax.axis_size(axis))])


def params(mib):
    return pltpu.CompilerParams(vmem_limit_bytes=int(mib * 1024) << 10)


def place():
    tok = lax.axis_index("tok")
    return tok >> 1, tok & 1, lax.axis_index("section")


def cost(flops, moved):
    return pl.CostEstimate(flops=int(flops), bytes_accessed=int(moved), transcendentals=0)


def deal_kernel(width, proj, mine, give):
    core = place()[1]
    rank, half = proj.shape[1], mine.shape[1]
    row = lax.broadcasted_iota(jnp.int32, (rank, half), 0)
    col = lax.broadcasted_iota(jnp.int32, (rank, half), 1)
    first = (col // width) * (2 * width) + col % width
    picks = [
        jnp.where(row == first + side * width, 1.0, 0.0).astype(BF16) for side in (core, 1 - core)
    ]
    for out, pick in zip((mine, give), picks):
        out[...] = jnp.dot(proj[...], pick, preferred_element_type=F32).astype(BF16)


def deal(proj, width):
    rows, rank = proj.shape
    half = jax.ShapeDtypeStruct((rows, rank // 2), BF16)
    return pl.pallas_call(
        functools.partial(deal_kernel, width),
        out_shape=(half, half),
        in_specs=[VMEM],
        out_specs=(VMEM, VMEM),
        compiler_params=params(4),
        cost_estimate=cost(2 * rows * rank * rank, 4 * rows * rank),
        name="deal",
    )(proj)


def stage_kernel(k, source, out, sem):
    deep = out.shape[1]
    columns = pl.ds(pl.multiple_of((place()[0] ^ k) * deep, 128), deep)
    copy = pltpu.make_async_copy(source.at[:, columns], out, sem)
    copy.start()
    copy.wait()


def stage(source, k, deep):
    rows = source.shape[0]
    return pl.pallas_call(
        functools.partial(stage_kernel, k),
        out_shape=jax.ShapeDtypeStruct((rows, deep), BF16),
        in_specs=[HBM],
        out_specs=VMEM,
        scratch_shapes=[pltpu.SemaphoreType.DMA],
        compiler_params=params(3),
        cost_estimate=cost(4e9, 4 * rows * deep),
        name="stage",
    )(source)


def join_kernel(upper, lower, out):
    deep = upper.shape[0]
    out[:deep, :] = upper[...]
    out[deep:, :] = lower[...]


def join(upper, lower):
    deep, half = upper.shape
    return pl.pallas_call(
        join_kernel,
        out_shape=jax.ShapeDtypeStruct((2 * deep, half), BF16),
        in_specs=[VMEM, VMEM],
        out_specs=VMEM,
        compiler_params=params(2),
        cost_estimate=cost(1e6, 8 * deep * half),
        name="join",
    )(upper, lower)


def pick_kernel(parts, j, upper, lower, out):
    deep = out.shape[0] // 2
    rows = pl.ds(pl.multiple_of(((place()[2] % parts) ^ j) * deep, 16), deep)
    out[:deep, :] = upper[rows, :]
    out[deep:, :] = lower[rows, :]


def pick(upper, lower, parts, j):
    rows, half = upper.shape
    return pl.pallas_call(
        functools.partial(pick_kernel, parts, j),
        out_shape=jax.ShapeDtypeStruct((2 * rows // parts, half), BF16),
        in_specs=[VMEM, VMEM],
        out_specs=VMEM,
        compiler_params=params(4),
        cost_estimate=cost(1e6, 8 * rows * half // parts),
        name="pick",
    )(upper, lower)


def project_kernel(groups, parts, started, last, layers, *refs):
    arrays, refs = refs[: 2 * len(groups)], refs[2 * len(groups) :]
    count = sum(len(keys) for keys in groups)
    pieces, refs = refs[:count], refs[count:]
    total = refs[0] if started else None
    outs = refs[started:]
    _, core, section = place()
    part = section % parts
    block = arrays[0].shape[1] // 2
    sides = (core, 1 - core)
    spots = []
    for n, keys in enumerate(groups):
        for j, which in keys:
            for side in which:
                if j is None:
                    spots.append((n, sides[side] * block, block))
                else:
                    at = sides[side] * block + (part ^ j) * (block // parts)
                    spots.append((n, at, block // parts))
    spots = [(n, pl.ds(pl.multiple_of(at, 128), deep)) for n, at, deep in spots]
    weights = jnp.concatenate([piece[...] for piece in pieces], axis=0)
    rows = arrays[0].shape[0] // layers
    kept = []
    for side in range(2):
        for layer in range(layers):
            span = pl.ds(layer * rows, rows)
            left = [arrays[2 * n + side][span, columns] for n, columns in spots]
            left = jnp.concatenate(left, axis=1)
            value = jnp.dot(left, weights, preferred_element_type=F32)
            if started:
                value = value + total[side, span, :]
            if last:
                kept.append(value)
            else:
                outs[0][side, span, :] = value
    if not last:
        return
    split, sums = outs
    sums[...] = jnp.zeros_like(sums)
    for layer in range(layers):
        values = [kept[layer], kept[layers + layer]]
        column = jnp.sum(values[0] + values[1], axis=0, keepdims=True)
        sums[layer : layer + 1, :] = column
        mean = column / (2 * rows)
        for side in range(2):
            span = pl.ds(layer * rows, rows)
            value = values[side] - mean
            high = value.astype(BF16)
            split[0, side, span, :] = high
            split[1, side, span, :] = (value - high.astype(F32)).astype(BF16)


def project(groups, parts, total, layers, last):
    arrays = [array for acts, _ in groups for array in acts]
    pieces = [piece for _, held in groups for piece in held.values()]
    keys = tuple(tuple(held) for _, held in groups)
    rows, half = arrays[0].shape[0], pieces[0].shape[1]
    deep = sum(piece.shape[0] for piece in pieces)
    if last:
        out_shape = (
            jax.ShapeDtypeStruct((2, 2, rows, half), BF16),
            jax.ShapeDtypeStruct((8, half), F32),
        )
        out_specs = (VMEM, VMEM)
    else:
        out_shape = jax.ShapeDtypeStruct((2, rows, half), F32)
        out_specs = VMEM
    started = [] if total is None else [total]
    return pl.pallas_call(
        functools.partial(project_kernel, keys, parts, len(started), last, layers),
        out_shape=out_shape,
        in_specs=[VMEM] * (len(arrays) + len(pieces) + len(started)),
        out_specs=out_specs,
        compiler_params=params(14 if len(groups) > 1 else 10),
        cost_estimate=cost(4 * rows * deep * half, 4 * rows * deep),
        name="project",
    )(*arrays, *pieces, *started)


def exponent(value):
    top = jnp.max(jnp.abs(value), axis=(0, 1), keepdims=True)
    return jnp.ceil(jnp.log2(jnp.maximum(top, 1e-30))) - 14.0


ALONG_TOKENS = (((0,), (0,)), ((), ()))


def halves(ref, layer, rows, swapped):
    span = pl.ds(layer * rows, rows)
    sides = (1, 0) if swapped else (0, 1)
    return [jnp.concatenate([ref[part, n, span, :] for n in sides], axis=0) for part in range(2)]


def outer(left, right):
    return sum(
        lax.dot_general(left[i], right[j], ALONG_TOKENS, preferred_element_type=F32)
        for i, j in ((0, 0), (0, 1), (1, 0))
    )


def inner_gram_kernel(layers, own, out):
    rows = own.shape[2] // layers
    for layer in range(layers):
        here = halves(own, layer, rows, False)
        out[layer] = outer(here, here)


def inner_gram(own, layers):
    rows, half = own.shape[2:]
    return pl.pallas_call(
        functools.partial(inner_gram_kernel, layers),
        out_shape=jax.ShapeDtypeStruct((layers, half, half), F32),
        in_specs=[VMEM],
        out_specs=VMEM,
        compiler_params=params(6),
        cost_estimate=cost(12 * rows * half * half, 16 * rows * half),
        name="inner_gram",
    )(own)


def gram_kernel(layers, chips, inner, own, oth, own_sums, oth_sums, *outs):
    chip = place()[0]
    half = own.shape[3]
    rows = own.shape[2] // layers
    width = half // chips
    sums = jnp.concatenate([own_sums[...], oth_sums[...]], axis=1)
    tail = []
    for layer in range(layers):
        cross = outer(halves(own, layer, rows, False), halves(oth, layer, rows, True))
        gram = jnp.concatenate([inner[layer], cross], axis=1)
        power = exponent(gram)
        gram = gram * jnp.exp2(-power)
        blocks = [gram[i * width : (i + 1) * width] for i in range(chips)]
        for k, out in enumerate(outs):
            block = blocks[k]
            for i in range(1, chips):
                block = jnp.where(chip == i, blocks[i ^ k], block)
            out[layer * width : (layer + 1) * width, :] = block
        column = sums[layer : layer + 1]
        lift = exponent(column)
        column = column * jnp.exp2(-lift)
        high = column.astype(BF16).astype(F32)
        middle = (column - high).astype(BF16).astype(F32)
        line = jnp.zeros((1, half), F32)
        powers = jnp.concatenate([line + power, line + lift], axis=1)
        tail += [high, middle, column - high - middle, powers]
    for out in outs:
        if len(tail) < tail_rows(layers):
            out[layers * width :, :] = jnp.zeros_like(out[layers * width :, :])
        for n, line in enumerate(tail):
            out[layers * width + n : layers * width + n + 1, :] = line


def tail_rows(layers):
    return -(-4 * layers // 8) * 8


def gram(inner, own, oth, own_sums, oth_sums, layers, chips):
    rows, half = own.shape[2:]
    height = layers * (half // chips) + tail_rows(layers)
    message = jax.ShapeDtypeStruct((height, 2 * half), F32)
    return pl.pallas_call(
        functools.partial(gram_kernel, layers, chips),
        out_shape=(message,) * chips,
        in_specs=[VMEM] * 5,
        out_specs=(VMEM,) * chips,
        compiler_params=params(10),
        cost_estimate=cost(12 * rows * half * half, 16 * rows * half),
        name="gram",
    )(inner, own, oth, own_sums, oth_sums)


def finish_kernel(layers, tokens, *refs):
    messages, (sketch, turned, first_out, second_out) = refs[:-4], refs[-4:]
    chips = len(messages)
    chip, core, section = place()
    rank = messages[0].shape[1]
    width = (messages[0].shape[0] - tail_rows(layers)) // layers
    half = rank // 2
    here = lax.broadcasted_iota(jnp.int32, (width, rank), 1)
    here = here == lax.broadcasted_iota(jnp.int32, (width, rank), 0) + chip * width
    kept = []
    for layer in range(layers):
        span = slice(layer * width, (layer + 1) * width)
        at = layers * width + 4 * layer
        value, sums = 0.0, []
        for message in messages:
            line = [message[at + n : at + n + 1, :] for n in range(4)]
            scale = jnp.exp2(line[3])
            value = value + message[span, :] * scale[:, :1]
            sums.append((line[0] + line[1] + line[2]) * scale[:, rank - 1 :])
        mean = sum(sums) / tokens
        for total in sums:
            drift = total / (tokens // chips) - mean
            lifted = jnp.sum(jnp.where(here, drift, 0.0), axis=1, keepdims=True)
            value = value + (tokens // chips) * lifted * drift
        turned[layer] = value
        kept.append(value)
        flipped = value.T
        for i in range(chips):
            for side in range(2):
                at = side * half + i * width
                to = 2 * width * i + width * (core if side == 0 else 1 - core)
                rows = pl.ds(pl.multiple_of(to, 8), width)
                sketch[layer, rows, :] = flipped[at : at + width]
    odd = section % 2 == 1
    first_out[...] = jnp.where(odd, kept[0], kept[-1]).astype(BF16)
    second_out[...] = jnp.where(odd, kept[-1], kept[0]).astype(BF16)


def finish(messages, layers, tokens):
    height, rank = messages[0].shape
    width = (height - tail_rows(layers)) // layers
    edge = jax.ShapeDtypeStruct((width, rank), BF16)
    return pl.pallas_call(
        functools.partial(finish_kernel, layers, tokens),
        out_shape=(
            jax.ShapeDtypeStruct((layers, rank, width), F32),
            jax.ShapeDtypeStruct((layers, width, rank), F32),
            edge,
            edge,
        ),
        in_specs=[VMEM] * len(messages),
        out_specs=(VMEM,) * 4,
        compiler_params=params(6),
        cost_estimate=cost(1e6, 2e6),
        name="finish",
    )(*messages)


def products_kernel(layers, sections, turned, one, two, out):
    section = place()[2]
    odd = section % 2 == 1
    one, two = one[...].astype(F32), two[...].astype(F32)
    rows = [turned[i] for i in range(layers)]
    before = jnp.where(section == 0, rows[0], jnp.where(odd, one, two))
    beyond = jnp.where(section == sections - 1, rows[-1], jnp.where(odd, two, one))
    pairs = [(before, before)] + [(row, row) for row in rows] + [(beyond, beyond)]
    chain = [before] + rows + [beyond]
    pairs += list(zip(chain[:-1], chain[1:]))
    out[...] = jnp.zeros_like(out)
    for n, (a, b) in enumerate(pairs):
        out[n : n + 1, :] = jnp.full((1, out.shape[1]), jnp.sum(a * b), F32)


def products(turned, one, two, sections):
    layers = turned.shape[0]
    count = -(-(2 * layers + 3) // 8) * 8
    return pl.pallas_call(
        functools.partial(products_kernel, layers, sections),
        out_shape=jax.ShapeDtypeStruct((count, 128), F32),
        in_specs=[VMEM] * 3,
        out_specs=VMEM,
        compiler_params=params(4),
        cost_estimate=cost(1e6, 1e6),
        name="products",
    )(turned, one, two)


def ratios_kernel(layers, *refs):
    out = refs[-1]
    value = sum(ref[...] for ref in refs[:-1])
    squares = value[: layers + 2]
    chained = value[layers + 2 : 2 * layers + 3]
    ratio = chained / jnp.sqrt(squares[:-1] * squares[1:])
    out[:, 0:1] = ratio[:-1, 0:1]
    out[:, 1:2] = ratio[1:, 0:1]


def ratios(shares, layers):
    return pl.pallas_call(
        functools.partial(ratios_kernel, layers),
        out_shape=jax.ShapeDtypeStruct((layers, 2), F32),
        in_specs=[VMEM] * len(shares),
        out_specs=VMEM,
        compiler_params=params(4),
        cost_estimate=cost(1e4, 1e4),
        name="ratios",
    )(*shares)


def local(activations, projection):
    layers, tok_rows, model = activations.shape
    block, rank = projection.shape
    groups, sections = lax.axis_size("tok"), lax.axis_size("section")
    chips, width = groups // 2, rank // groups
    parts = min(sections, max(1, block // 128))
    deep = block // parts

    acts = activations.reshape(layers * tok_rows, model)
    start = (lax.axis_index("section") & (parts - 1)) * deep
    part = lax.dynamic_slice_in_dim(projection, start, deep, 0)
    mine_part, give_part = deal(part, width)
    got_part = swap(give_part, "tok", 1)
    own = join(mine_part, got_part)

    fetched = {}
    for k in range(1, chips):
        low = k & -k
        fetched[k] = swap(own if k == low else fetched[k ^ low], "tok", 2 * low)

    mine, give = deal(projection, width)
    got = swap(give, "tok", 1)

    order = sorted(fetched, key=lambda k: (bin(k).count("1"), k))
    staged = {}
    for k in [0] + order:
        staged[k] = stage(acts, k, 2 * block)
        staged[k] = (staged[k], swap(staged[k], "tok", 1))

    far = {j: pick(mine, got, parts, j) for j in range(1, parts) if j & (j - 1)}
    both, final = (0, 1), order[-1]
    pieces = {}
    for k in order:
        held = {(0, both): fetched[k]}
        for j in range(1, parts):
            near = j & -j
            if j in far and k in (1, final):
                held[j, both] = swap(far[j], "tok", 2 * k)
            elif j in far and (j ^ near) not in far:
                upper = swap(held[j ^ near, both][:deep], "section", near)
                lower = swap(held[near, both][deep:], "section", j ^ near)
                held[j, (0,)], held[j, (1,)] = upper, lower
            else:
                held[j, both] = swap(fetched[k], "section", j)
        pieces[k] = held

    own_rows = {(None, (0,)): mine, (None, (1,)): got}
    total = project([(staged[0], own_rows)], parts, None, layers, False)

    def is_late(k, key):
        return len(key[1]) == 1 or (k == final and key[0] != 0 and key[0] not in far)

    late, early = [], {}
    for k in order:
        early[k] = {key: piece for key, piece in pieces[k].items() if not is_late(k, key)}
        held = {key: piece for key, piece in pieces[k].items() if is_late(k, key)}
        if held:
            late.append((staged[k], held))
    steps = [(k, [(staged[k], early[k])]) for k in order[-2::-1] + order[-1:]]
    if late:
        steps.append((None, late))
    for n, (k, groups_of) in enumerate(steps):
        last = n == len(steps) - 1
        total = project(groups_of, parts, total, layers, last)
    split, sums = total

    split_oth = swap(split, "tok", 1)
    sums_oth = swap(sums, "tok", 1)
    inner = inner_gram(split, layers)
    messages = gram(inner, split, split_oth, sums, sums_oth, layers, chips)
    arrived = [messages[0]]
    for k in reversed(range(1, chips)):
        arrived.append(swap(messages[k].astype(jnp.float16), "tok", 2 * k).astype(F32))
    sketch, turned, first, second = finish(arrived, layers, tok_rows * groups)

    route = [(i, i + 1) for i in range(1, sections - 1, 2)]
    second = lax.ppermute(second, "section", route + [(b, a) for a, b in route])
    first = swap(first, "section", 1)
    value = products(turned, first, second, sections)
    value = value + swap(value, "tok", 1)
    if chips <= 4:
        others = []
        for k in reversed(range(1, chips)):
            others.append(swap(value, "tok", 2 * k))
    else:
        mask = 2
        while 2 * mask < groups:
            value = value + swap(value, "tok", mask)
            mask *= 2
        others = [swap(value, "tok", mask)]
    return sketch, ratios([value] + others, layers)


def solution(mesh):
    return jax.shard_map(
        local,
        mesh=mesh,
        in_specs=(P("section", "tok", None), P("tok", None)),
        out_specs=(P("section", None, "tok"), P("section", None)),
        check_vma=False,
    )
```

```python
import functools

import jax
import jax.numpy as jnp
from jax import lax
from jax.experimental import pallas as pl
from jax.experimental.pallas import tpu as pltpu
from jax.sharding import PartitionSpec as P


F32, BF16 = jnp.float32, jnp.bfloat16
VMEM = pl.BlockSpec(memory_space=pltpu.VMEM)
HBM = pl.BlockSpec(memory_space=pltpu.HBM)


def swap(block, axis, mask):
    return lax.ppermute(block, axis, [(i, i ^ mask) for i in range(lax.axis_size(axis))])


def params(mib):
    return pltpu.CompilerParams(vmem_limit_bytes=int(mib * 1024) << 10)


def place():
    tok = lax.axis_index("tok")
    return tok >> 1, tok & 1, lax.axis_index("section")


def cost(flops, moved):
    return pl.CostEstimate(flops=int(flops), bytes_accessed=int(moved), transcendentals=0)


def deal_kernel(width, proj, mine, give):
    core = place()[1]
    rank, half = proj.shape[1], mine.shape[1]
    row = lax.broadcasted_iota(jnp.int32, (rank, half), 0)
    col = lax.broadcasted_iota(jnp.int32, (rank, half), 1)
    first = (col // width) * (2 * width) + col % width
    picks = [
        jnp.where(row == first + side * width, 1.0, 0.0).astype(BF16) for side in (core, 1 - core)
    ]
    for out, pick in zip((mine, give), picks):
        out[...] = jnp.dot(proj[...], pick, preferred_element_type=F32).astype(BF16)


def deal(proj, width):
    rows, rank = proj.shape
    half = jax.ShapeDtypeStruct((rows, rank // 2), BF16)
    return pl.pallas_call(
        functools.partial(deal_kernel, width),
        out_shape=(half, half),
        in_specs=[VMEM],
        out_specs=(VMEM, VMEM),
        compiler_params=params(4),
        cost_estimate=cost(2 * rows * rank * rank, 4 * rows * rank),
        name="deal",
    )(proj)


def stage_kernel(k, source, out, sem):
    deep = out.shape[1]
    columns = pl.ds(pl.multiple_of((place()[0] ^ k) * deep, 128), deep)
    copy = pltpu.make_async_copy(source.at[:, columns], out, sem)
    copy.start()
    copy.wait()


def stage(source, k, deep):
    rows = source.shape[0]
    return pl.pallas_call(
        functools.partial(stage_kernel, k),
        out_shape=jax.ShapeDtypeStruct((rows, deep), BF16),
        in_specs=[HBM],
        out_specs=VMEM,
        scratch_shapes=[pltpu.SemaphoreType.DMA],
        compiler_params=params(3),
        cost_estimate=cost(4e9, 4 * rows * deep),
        name="stage",
    )(source)


def join_kernel(upper, lower, out):
    deep = upper.shape[0]
    out[:deep, :] = upper[...]
    out[deep:, :] = lower[...]


def join(upper, lower):
    deep, half = upper.shape
    return pl.pallas_call(
        join_kernel,
        out_shape=jax.ShapeDtypeStruct((2 * deep, half), BF16),
        in_specs=[VMEM, VMEM],
        out_specs=VMEM,
        compiler_params=params(2),
        cost_estimate=cost(1e6, 8 * deep * half),
        name="join",
    )(upper, lower)


def pick_kernel(parts, j, upper, lower, out):
    deep = out.shape[0] // 2
    rows = pl.ds(pl.multiple_of(((place()[2] % parts) ^ j) * deep, 16), deep)
    out[:deep, :] = upper[rows, :]
    out[deep:, :] = lower[rows, :]


def pick(upper, lower, parts, j):
    rows, half = upper.shape
    return pl.pallas_call(
        functools.partial(pick_kernel, parts, j),
        out_shape=jax.ShapeDtypeStruct((2 * rows // parts, half), BF16),
        in_specs=[VMEM, VMEM],
        out_specs=VMEM,
        compiler_params=params(4),
        cost_estimate=cost(1e6, 8 * rows * half // parts),
        name="pick",
    )(upper, lower)


def project_kernel(groups, parts, started, last, layers, *refs):
    arrays, refs = refs[: 2 * len(groups)], refs[2 * len(groups) :]
    count = sum(len(keys) for keys in groups)
    pieces, refs = refs[:count], refs[count:]
    total = refs[0] if started else None
    outs = refs[started:]
    _, core, section = place()
    part = section % parts
    block = arrays[0].shape[1] // 2
    sides = (core, 1 - core)
    spots = []
    for n, keys in enumerate(groups):
        for j, which in keys:
            for side in which:
                if j is None:
                    spots.append((n, sides[side] * block, block))
                else:
                    at = sides[side] * block + (part ^ j) * (block // parts)
                    spots.append((n, at, block // parts))
    spots = [(n, pl.ds(pl.multiple_of(at, 128), deep)) for n, at, deep in spots]
    weights = jnp.concatenate([piece[...] for piece in pieces], axis=0)
    rows = arrays[0].shape[0] // layers
    kept = []
    for side in range(2):
        for layer in range(layers):
            span = pl.ds(layer * rows, rows)
            left = [arrays[2 * n + side][span, columns] for n, columns in spots]
            left = jnp.concatenate(left, axis=1)
            value = jnp.dot(left, weights, preferred_element_type=F32)
            if started:
                value = value + total[side, span, :]
            if last:
                kept.append(value)
            else:
                outs[0][side, span, :] = value
    if not last:
        return
    split, sums = outs
    sums[...] = jnp.zeros_like(sums)
    for layer in range(layers):
        values = [kept[layer], kept[layers + layer]]
        column = jnp.sum(values[0] + values[1], axis=0, keepdims=True)
        sums[layer : layer + 1, :] = column
        mean = column / (2 * rows)
        for side in range(2):
            span = pl.ds(layer * rows, rows)
            value = values[side] - mean
            high = value.astype(BF16)
            split[0, side, span, :] = high
            split[1, side, span, :] = (value - high.astype(F32)).astype(BF16)


def project(groups, parts, total, layers, last):
    arrays = [array for acts, _ in groups for array in acts]
    pieces = [piece for _, held in groups for piece in held.values()]
    keys = tuple(tuple(held) for _, held in groups)
    rows, half = arrays[0].shape[0], pieces[0].shape[1]
    deep = sum(piece.shape[0] for piece in pieces)
    if last:
        out_shape = (
            jax.ShapeDtypeStruct((2, 2, rows, half), BF16),
            jax.ShapeDtypeStruct((8, half), F32),
        )
        out_specs = (VMEM, VMEM)
    else:
        out_shape = jax.ShapeDtypeStruct((2, rows, half), F32)
        out_specs = VMEM
    started = [] if total is None else [total]
    return pl.pallas_call(
        functools.partial(project_kernel, keys, parts, len(started), last, layers),
        out_shape=out_shape,
        in_specs=[VMEM] * (len(arrays) + len(pieces) + len(started)),
        out_specs=out_specs,
        compiler_params=params(14 if len(groups) > 1 else 10),
        cost_estimate=cost(4 * rows * deep * half, 4 * rows * deep),
        name="project",
    )(*arrays, *pieces, *started)


def exponent(value):
    top = jnp.max(jnp.abs(value), axis=(0, 1), keepdims=True)
    return jnp.ceil(jnp.log2(jnp.maximum(top, 1e-30))) - 14.0


ALONG_TOKENS = (((0,), (0,)), ((), ()))


def halves(ref, layer, rows, swapped):
    span = pl.ds(layer * rows, rows)
    sides = (1, 0) if swapped else (0, 1)
    return [jnp.concatenate([ref[part, n, span, :] for n in sides], axis=0) for part in range(2)]


def outer(left, right):
    return sum(
        lax.dot_general(left[i], right[j], ALONG_TOKENS, preferred_element_type=F32)
        for i, j in ((0, 0), (0, 1), (1, 0))
    )


def inner_gram_kernel(layers, own, out):
    rows = own.shape[2] // layers
    for layer in range(layers):
        here = halves(own, layer, rows, False)
        out[layer] = outer(here, here)


def inner_gram(own, layers):
    rows, half = own.shape[2:]
    return pl.pallas_call(
        functools.partial(inner_gram_kernel, layers),
        out_shape=jax.ShapeDtypeStruct((layers, half, half), F32),
        in_specs=[VMEM],
        out_specs=VMEM,
        compiler_params=params(6),
        cost_estimate=cost(12 * rows * half * half, 16 * rows * half),
        name="inner_gram",
    )(own)


def gram_kernel(layers, chips, inner, own, oth, own_sums, oth_sums, *outs):
    chip = place()[0]
    half = own.shape[3]
    rows = own.shape[2] // layers
    width = half // chips
    sums = jnp.concatenate([own_sums[...], oth_sums[...]], axis=1)
    tail = []
    for layer in range(layers):
        cross = outer(halves(own, layer, rows, False), halves(oth, layer, rows, True))
        gram = jnp.concatenate([inner[layer], cross], axis=1)
        power = exponent(gram)
        gram = gram * jnp.exp2(-power)
        blocks = [gram[i * width : (i + 1) * width] for i in range(chips)]
        for k, out in enumerate(outs):
            block = blocks[k]
            for i in range(1, chips):
                block = jnp.where(chip == i, blocks[i ^ k], block)
            out[layer * width : (layer + 1) * width, :] = block
        column = sums[layer : layer + 1]
        lift = exponent(column)
        column = column * jnp.exp2(-lift)
        high = column.astype(BF16).astype(F32)
        middle = (column - high).astype(BF16).astype(F32)
        line = jnp.zeros((1, half), F32)
        powers = jnp.concatenate([line + power, line + lift], axis=1)
        tail += [high, middle, column - high - middle, powers]
    for out in outs:
        if len(tail) < tail_rows(layers):
            out[layers * width :, :] = jnp.zeros_like(out[layers * width :, :])
        for n, line in enumerate(tail):
            out[layers * width + n : layers * width + n + 1, :] = line


def tail_rows(layers):
    return -(-4 * layers // 8) * 8


def gram(inner, own, oth, own_sums, oth_sums, layers, chips):
    rows, half = own.shape[2:]
    height = layers * (half // chips) + tail_rows(layers)
    message = jax.ShapeDtypeStruct((height, 2 * half), F32)
    return pl.pallas_call(
        functools.partial(gram_kernel, layers, chips),
        out_shape=(message,) * chips,
        in_specs=[VMEM] * 5,
        out_specs=(VMEM,) * chips,
        compiler_params=params(10),
        cost_estimate=cost(12 * rows * half * half, 16 * rows * half),
        name="gram",
    )(inner, own, oth, own_sums, oth_sums)


def finish_kernel(layers, tokens, *refs):
    messages, (sketch, turned, first_out, second_out) = refs[:-4], refs[-4:]
    chips = len(messages)
    chip, core, section = place()
    rank = messages[0].shape[1]
    width = (messages[0].shape[0] - tail_rows(layers)) // layers
    half = rank // 2
    here = lax.broadcasted_iota(jnp.int32, (width, rank), 1)
    here = here == lax.broadcasted_iota(jnp.int32, (width, rank), 0) + chip * width
    kept = []
    for layer in range(layers):
        span = slice(layer * width, (layer + 1) * width)
        at = layers * width + 4 * layer
        value, sums = 0.0, []
        for message in messages:
            line = [message[at + n : at + n + 1, :] for n in range(4)]
            scale = jnp.exp2(line[3])
            value = value + message[span, :] * scale[:, :1]
            sums.append((line[0] + line[1] + line[2]) * scale[:, rank - 1 :])
        mean = sum(sums) / tokens
        for total in sums:
            drift = total / (tokens // chips) - mean
            lifted = jnp.sum(jnp.where(here, drift, 0.0), axis=1, keepdims=True)
            value = value + (tokens // chips) * lifted * drift
        turned[layer] = value
        kept.append(value)
        flipped = value.T
        for i in range(chips):
            for side in range(2):
                at = side * half + i * width
                to = 2 * width * i + width * (core if side == 0 else 1 - core)
                rows = pl.ds(pl.multiple_of(to, 8), width)
                sketch[layer, rows, :] = flipped[at : at + width]
    odd = section % 2 == 1
    first_out[...] = jnp.where(odd, kept[0], kept[-1]).astype(BF16)
    second_out[...] = jnp.where(odd, kept[-1], kept[0]).astype(BF16)


def finish(messages, layers, tokens):
    height, rank = messages[0].shape
    width = (height - tail_rows(layers)) // layers
    edge = jax.ShapeDtypeStruct((width, rank), BF16)
    return pl.pallas_call(
        functools.partial(finish_kernel, layers, tokens),
        out_shape=(
            jax.ShapeDtypeStruct((layers, rank, width), F32),
            jax.ShapeDtypeStruct((layers, width, rank), F32),
            edge,
            edge,
        ),
        in_specs=[VMEM] * len(messages),
        out_specs=(VMEM,) * 4,
        compiler_params=params(6),
        cost_estimate=cost(1e6, 2e6),
        name="finish",
    )(*messages)


def products_kernel(layers, sections, turned, one, two, out):
    section = place()[2]
    odd = section % 2 == 1
    one, two = one[...].astype(F32), two[...].astype(F32)
    rows = [turned[i] for i in range(layers)]
    before = jnp.where(section == 0, rows[0], jnp.where(odd, one, two))
    beyond = jnp.where(section == sections - 1, rows[-1], jnp.where(odd, two, one))
    pairs = [(before, before)] + [(row, row) for row in rows] + [(beyond, beyond)]
    chain = [before] + rows + [beyond]
    pairs += list(zip(chain[:-1], chain[1:]))
    out[...] = jnp.zeros_like(out)
    for n, (a, b) in enumerate(pairs):
        out[n : n + 1, :] = jnp.full((1, out.shape[1]), jnp.sum(a * b), F32)


def products(turned, one, two, sections):
    layers = turned.shape[0]
    count = -(-(2 * layers + 3) // 8) * 8
    return pl.pallas_call(
        functools.partial(products_kernel, layers, sections),
        out_shape=jax.ShapeDtypeStruct((count, 128), F32),
        in_specs=[VMEM] * 3,
        out_specs=VMEM,
        compiler_params=params(4),
        cost_estimate=cost(1e6, 1e6),
        name="products",
    )(turned, one, two)


def ratios_kernel(layers, *refs):
    out = refs[-1]
    value = sum(ref[...] for ref in refs[:-1])
    squares = value[: layers + 2]
    chained = value[layers + 2 : 2 * layers + 3]
    ratio = chained / jnp.sqrt(squares[:-1] * squares[1:])
    out[:, 0:1] = ratio[:-1, 0:1]
    out[:, 1:2] = ratio[1:, 0:1]


def ratios(shares, layers):
    return pl.pallas_call(
        functools.partial(ratios_kernel, layers),
        out_shape=jax.ShapeDtypeStruct((layers, 2), F32),
        in_specs=[VMEM] * len(shares),
        out_specs=VMEM,
        compiler_params=params(4),
        cost_estimate=cost(1e4, 1e4),
        name="ratios",
    )(*shares)


def local(activations, projection):
    layers, tok_rows, model = activations.shape
    block, rank = projection.shape
    groups, sections = lax.axis_size("tok"), lax.axis_size("section")
    chips, width = groups // 2, rank // groups
    parts = min(sections, max(1, block // 128))
    deep = block // parts

    acts = activations.reshape(layers * tok_rows, model)
    start = (lax.axis_index("section") & (parts - 1)) * deep
    part = lax.dynamic_slice_in_dim(projection, start, deep, 0)
    mine_part, give_part = deal(part, width)
    got_part = swap(give_part, "tok", 1)
    own = join(mine_part, got_part)

    fetched = {}
    for k in range(1, chips):
        low = k & -k
        fetched[k] = swap(own if k == low else fetched[k ^ low], "tok", 2 * low)

    mine, give = deal(projection, width)
    got = swap(give, "tok", 1)

    order = sorted(fetched, key=lambda k: (bin(k).count("1"), k))
    staged = {}
    for k in [0] + order:
        staged[k] = stage(acts, k, 2 * block)
        staged[k] = (staged[k], swap(staged[k], "tok", 1))

    far = {j: pick(mine, got, parts, j) for j in range(1, parts) if j & (j - 1)}
    both, final = (0, 1), order[-1]
    pieces = {}
    for k in order:
        held = {(0, both): fetched[k]}
        for j in range(1, parts):
            near = j & -j
            if j in far and k in (1, final):
                held[j, both] = swap(far[j], "tok", 2 * k)
            elif j in far and (j ^ near) not in far:
                upper = swap(held[j ^ near, both][:deep], "section", near)
                lower = swap(held[near, both][deep:], "section", j ^ near)
                held[j, (0,)], held[j, (1,)] = upper, lower
            else:
                held[j, both] = swap(fetched[k], "section", j)
        pieces[k] = held

    own_rows = {(None, (0,)): mine, (None, (1,)): got}
    total = project([(staged[0], own_rows)], parts, None, layers, False)

    def held_by(k, kind):
        return {key: piece for key, piece in pieces[k].items() if kind(*key)}

    def is_far(j, which):
        return j in far and len(which) == 2

    near = {k: held_by(k, lambda j, which: j not in far) for k in order}
    passed = [(staged[k], held_by(k, lambda j, which: len(which) == 1)) for k in order]
    distant = [(staged[k], held_by(k, is_far)) for k in order]
    steps = [(f"acc{k}", [(staged[k], near[k])]) for k in order[-2::-1]]
    steps.append((f"acc{final}", [(staged[final], near[final])]))
    steps.append(("last", distant + passed))
    steps = [(name, [group for group in groups_of if group[1]]) for name, groups_of in steps]
    steps = [step for step in steps if step[1]]
    for name, groups_of in steps:
        last = name == steps[-1][0]
        total = project(groups_of, parts, total, layers, last)
    split, sums = total

    split_oth = swap(split, "tok", 1)
    sums_oth = swap(sums, "tok", 1)
    inner = inner_gram(split, layers)
    messages = gram(inner, split, split_oth, sums, sums_oth, layers, chips)
    arrived = [messages[0]]
    for k in reversed(range(1, chips)):
        arrived.append(swap(messages[k].astype(jnp.float16), "tok", 2 * k).astype(F32))
    sketch, turned, first, second = finish(arrived, layers, tok_rows * groups)

    route = [(i, i + 1) for i in range(1, sections - 1, 2)]
    second = lax.ppermute(second, "section", route + [(b, a) for a, b in route])
    first = swap(first, "section", 1)
    value = products(turned, first, second, sections)
    value = value + swap(value, "tok", 1)
    if chips <= 4:
        others = []
        for k in reversed(range(1, chips)):
            others.append(swap(value, "tok", 2 * k))
    else:
        mask = 2
        while 2 * mask < groups:
            value = value + swap(value, "tok", mask)
            mask *= 2
        others = [swap(value, "tok", mask)]
    return sketch, ratios([value] + others, layers)


def solution(mesh):
    return jax.shard_map(
        local,
        mesh=mesh,
        in_specs=(P("section", "tok", None), P("tok", None)),
        out_specs=(P("section", None, "tok"), P("section", None)),
        check_vma=False,
    )
```

```python
import functools

import jax
import jax.numpy as jnp
from jax import lax
from jax.experimental import pallas as pl
from jax.experimental.pallas import tpu as pltpu
from jax.sharding import PartitionSpec as P


F32, BF16 = jnp.float32, jnp.bfloat16
VMEM = pl.BlockSpec(memory_space=pltpu.VMEM)
HBM = pl.BlockSpec(memory_space=pltpu.HBM)


def swap(block, axis, mask):
    return lax.ppermute(block, axis, [(i, i ^ mask) for i in range(lax.axis_size(axis))])


def params(mib):
    return pltpu.CompilerParams(vmem_limit_bytes=int(mib * 1024) << 10)


def place():
    tok = lax.axis_index("tok")
    return tok >> 1, tok & 1, lax.axis_index("section")


def cost(flops, moved):
    return pl.CostEstimate(flops=int(flops), bytes_accessed=int(moved), transcendentals=0)


def deal_kernel(width, proj, mine, give):
    core = place()[1]
    rank, half = proj.shape[1], mine.shape[1]
    row = lax.broadcasted_iota(jnp.int32, (rank, half), 0)
    col = lax.broadcasted_iota(jnp.int32, (rank, half), 1)
    first = (col // width) * (2 * width) + col % width
    picks = [
        jnp.where(row == first + side * width, 1.0, 0.0).astype(BF16) for side in (core, 1 - core)
    ]
    for out, pick in zip((mine, give), picks):
        out[...] = jnp.dot(proj[...], pick, preferred_element_type=F32).astype(BF16)


def deal(proj, width):
    rows, rank = proj.shape
    half = jax.ShapeDtypeStruct((rows, rank // 2), BF16)
    return pl.pallas_call(
        functools.partial(deal_kernel, width),
        out_shape=(half, half),
        in_specs=[VMEM],
        out_specs=(VMEM, VMEM),
        compiler_params=params(4),
        cost_estimate=cost(2 * rows * rank * rank, 4 * rows * rank),
        name="deal",
    )(proj)


def stage_kernel(k, source, out, sem):
    deep = out.shape[1]
    columns = pl.ds(pl.multiple_of((place()[0] ^ k) * deep, 128), deep)
    copy = pltpu.make_async_copy(source.at[:, columns], out, sem)
    copy.start()
    copy.wait()


def stage(source, k, deep):
    rows = source.shape[0]
    return pl.pallas_call(
        functools.partial(stage_kernel, k),
        out_shape=jax.ShapeDtypeStruct((rows, deep), BF16),
        in_specs=[HBM],
        out_specs=VMEM,
        scratch_shapes=[pltpu.SemaphoreType.DMA],
        compiler_params=params(3),
        cost_estimate=cost(4e9, 4 * rows * deep),
        name="stage",
    )(source)


def join_kernel(upper, lower, out):
    deep = upper.shape[0]
    out[:deep, :] = upper[...]
    out[deep:, :] = lower[...]


def join(upper, lower):
    deep, half = upper.shape
    return pl.pallas_call(
        join_kernel,
        out_shape=jax.ShapeDtypeStruct((2 * deep, half), BF16),
        in_specs=[VMEM, VMEM],
        out_specs=VMEM,
        compiler_params=params(2),
        cost_estimate=cost(1e6, 8 * deep * half),
        name="join",
    )(upper, lower)


def pick_kernel(parts, j, upper, lower, out):
    deep = out.shape[0] // 2
    rows = pl.ds(pl.multiple_of(((place()[2] % parts) ^ j) * deep, 16), deep)
    out[:deep, :] = upper[rows, :]
    out[deep:, :] = lower[rows, :]


def pick(upper, lower, parts, j):
    rows, half = upper.shape
    return pl.pallas_call(
        functools.partial(pick_kernel, parts, j),
        out_shape=jax.ShapeDtypeStruct((2 * rows // parts, half), BF16),
        in_specs=[VMEM, VMEM],
        out_specs=VMEM,
        compiler_params=params(4),
        cost_estimate=cost(1e6, 8 * rows * half // parts),
        name="pick",
    )(upper, lower)


def project_kernel(groups, parts, started, last, layers, *refs):
    arrays, refs = refs[: 2 * len(groups)], refs[2 * len(groups) :]
    count = sum(len(keys) for keys in groups)
    pieces, refs = refs[:count], refs[count:]
    total = refs[0] if started else None
    outs = refs[started:]
    _, core, section = place()
    part = section % parts
    block = arrays[0].shape[1] // 2
    sides = (core, 1 - core)
    spots = []
    for n, keys in enumerate(groups):
        for j, which in keys:
            for side in which:
                if j is None:
                    spots.append((n, sides[side] * block, block))
                else:
                    at = sides[side] * block + (part ^ j) * (block // parts)
                    spots.append((n, at, block // parts))
    spots = [(n, pl.ds(pl.multiple_of(at, 128), deep)) for n, at, deep in spots]
    weights = jnp.concatenate([piece[...] for piece in pieces], axis=0)
    rows = arrays[0].shape[0] // layers
    kept = []
    for side in range(2):
        for layer in range(layers):
            span = pl.ds(layer * rows, rows)
            left = [arrays[2 * n + side][span, columns] for n, columns in spots]
            left = jnp.concatenate(left, axis=1)
            value = jnp.dot(left, weights, preferred_element_type=F32)
            if started:
                value = value + total[side, span, :]
            if last:
                kept.append(value)
            else:
                outs[0][side, span, :] = value
    if not last:
        return
    split, sums = outs
    sums[...] = jnp.zeros_like(sums)
    for layer in range(layers):
        values = [kept[layer], kept[layers + layer]]
        column = jnp.sum(values[0] + values[1], axis=0, keepdims=True)
        sums[layer : layer + 1, :] = column
        mean = column / (2 * rows)
        for side in range(2):
            span = pl.ds(layer * rows, rows)
            value = values[side] - mean
            high = value.astype(BF16)
            split[0, side, span, :] = high
            split[1, side, span, :] = (value - high.astype(F32)).astype(BF16)


def project(groups, parts, total, layers, last):
    arrays = [array for acts, _ in groups for array in acts]
    pieces = [piece for _, held in groups for piece in held.values()]
    keys = tuple(tuple(held) for _, held in groups)
    rows, half = arrays[0].shape[0], pieces[0].shape[1]
    deep = sum(piece.shape[0] for piece in pieces)
    if last:
        out_shape = (
            jax.ShapeDtypeStruct((2, 2, rows, half), BF16),
            jax.ShapeDtypeStruct((8, half), F32),
        )
        out_specs = (VMEM, VMEM)
    else:
        out_shape = jax.ShapeDtypeStruct((2, rows, half), F32)
        out_specs = VMEM
    started = [] if total is None else [total]
    return pl.pallas_call(
        functools.partial(project_kernel, keys, parts, len(started), last, layers),
        out_shape=out_shape,
        in_specs=[VMEM] * (len(arrays) + len(pieces) + len(started)),
        out_specs=out_specs,
        compiler_params=params(14 if len(groups) > 1 else 10),
        cost_estimate=cost(4 * rows * deep * half, 4 * rows * deep),
        name="project",
    )(*arrays, *pieces, *started)


def exponent(value):
    top = jnp.max(jnp.abs(value), axis=(0, 1), keepdims=True)
    return jnp.ceil(jnp.log2(jnp.maximum(top, 1e-30))) - 14.0


ALONG_TOKENS = (((0,), (0,)), ((), ()))


def halves(ref, layer, rows, swapped):
    span = pl.ds(layer * rows, rows)
    sides = (1, 0) if swapped else (0, 1)
    return [jnp.concatenate([ref[part, n, span, :] for n in sides], axis=0) for part in range(2)]


def outer(left, right):
    return sum(
        lax.dot_general(left[i], right[j], ALONG_TOKENS, preferred_element_type=F32)
        for i, j in ((0, 0), (0, 1), (1, 0))
    )


def inner_gram_kernel(layers, own, out):
    rows = own.shape[2] // layers
    for layer in range(layers):
        here = halves(own, layer, rows, False)
        out[layer] = outer(here, here)


def inner_gram(own, layers):
    rows, half = own.shape[2:]
    return pl.pallas_call(
        functools.partial(inner_gram_kernel, layers),
        out_shape=jax.ShapeDtypeStruct((layers, half, half), F32),
        in_specs=[VMEM],
        out_specs=VMEM,
        compiler_params=params(6),
        cost_estimate=cost(12 * rows * half * half, 16 * rows * half),
        name="inner_gram",
    )(own)


def gram_kernel(layers, chips, inner, own, oth, own_sums, oth_sums, *outs):
    chip = place()[0]
    half = own.shape[3]
    rows = own.shape[2] // layers
    width = half // chips
    sums = jnp.concatenate([own_sums[...], oth_sums[...]], axis=1)
    tail = []
    for layer in range(layers):
        cross = outer(halves(own, layer, rows, False), halves(oth, layer, rows, True))
        gram = jnp.concatenate([inner[layer], cross], axis=1)
        power = exponent(gram)
        gram = gram * jnp.exp2(-power)
        blocks = [gram[i * width : (i + 1) * width] for i in range(chips)]
        for k, out in enumerate(outs):
            block = blocks[k]
            for i in range(1, chips):
                block = jnp.where(chip == i, blocks[i ^ k], block)
            out[layer * width : (layer + 1) * width, :] = block
        column = sums[layer : layer + 1]
        lift = exponent(column)
        column = column * jnp.exp2(-lift)
        high = column.astype(BF16).astype(F32)
        middle = (column - high).astype(BF16).astype(F32)
        line = jnp.zeros((1, half), F32)
        powers = jnp.concatenate([line + power, line + lift], axis=1)
        tail += [high, middle, column - high - middle, powers]
    for out in outs:
        if len(tail) < tail_rows(layers):
            out[layers * width :, :] = jnp.zeros_like(out[layers * width :, :])
        for n, line in enumerate(tail):
            out[layers * width + n : layers * width + n + 1, :] = line


def tail_rows(layers):
    return -(-4 * layers // 8) * 8


def gram(inner, own, oth, own_sums, oth_sums, layers, chips):
    rows, half = own.shape[2:]
    height = layers * (half // chips) + tail_rows(layers)
    message = jax.ShapeDtypeStruct((height, 2 * half), F32)
    return pl.pallas_call(
        functools.partial(gram_kernel, layers, chips),
        out_shape=(message,) * chips,
        in_specs=[VMEM] * 5,
        out_specs=(VMEM,) * chips,
        compiler_params=params(10),
        cost_estimate=cost(12 * rows * half * half, 16 * rows * half),
        name="gram",
    )(inner, own, oth, own_sums, oth_sums)


def finish_kernel(layers, tokens, *refs):
    messages, (turned, first_out, second_out) = refs[:-3], refs[-3:]
    chips = len(messages)
    chip, _, section = place()
    rank = messages[0].shape[1]
    width = (messages[0].shape[0] - tail_rows(layers)) // layers
    here = lax.broadcasted_iota(jnp.int32, (width, rank), 1)
    here = here == lax.broadcasted_iota(jnp.int32, (width, rank), 0) + chip * width
    kept = []
    for layer in range(layers):
        span = slice(layer * width, (layer + 1) * width)
        at = layers * width + 4 * layer
        value, sums = 0.0, []
        for message in messages:
            line = [message[at + n : at + n + 1, :] for n in range(4)]
            scale = jnp.exp2(line[3])
            value = value + message[span, :] * scale[:, :1]
            sums.append((line[0] + line[1] + line[2]) * scale[:, rank - 1 :])
        mean = sum(sums) / tokens
        for total in sums:
            drift = total / (tokens // chips) - mean
            lifted = jnp.sum(jnp.where(here, drift, 0.0), axis=1, keepdims=True)
            value = value + (tokens // chips) * lifted * drift
        turned[layer] = value
        kept.append(value)
    odd = section % 2 == 1
    first_out[...] = jnp.where(odd, kept[0], kept[-1]).astype(BF16)
    second_out[...] = jnp.where(odd, kept[-1], kept[0]).astype(BF16)


def finish(messages, layers, tokens):
    height, rank = messages[0].shape
    width = (height - tail_rows(layers)) // layers
    edge = jax.ShapeDtypeStruct((width, rank), BF16)
    return pl.pallas_call(
        functools.partial(finish_kernel, layers, tokens),
        out_shape=(
            jax.ShapeDtypeStruct((layers, width, rank), F32),
            edge,
            edge,
        ),
        in_specs=[VMEM] * len(messages),
        out_specs=(VMEM,) * 3,
        compiler_params=params(6),
        cost_estimate=cost(1e6, 2e6),
        name="finish",
    )(*messages)


def upright_kernel(turned, sketch):
    core = place()[1]
    layers, width, rank = turned.shape
    for layer in range(layers):
        flipped = turned[layer].T
        for i in range(rank // (2 * width)):
            for side in range(2):
                at = side * (rank // 2) + i * width
                to = 2 * width * i + width * (core if side == 0 else 1 - core)
                rows = pl.ds(pl.multiple_of(to, 8), width)
                sketch[layer, rows, :] = flipped[at : at + width]


def upright(turned):
    layers, width, rank = turned.shape
    return pl.pallas_call(
        upright_kernel,
        out_shape=jax.ShapeDtypeStruct((layers, rank, width), F32),
        in_specs=[VMEM],
        out_specs=VMEM,
        compiler_params=params(6),
        cost_estimate=cost(1e6, 2e6),
        name="upright",
    )(turned)


def products_kernel(layers, sections, turned, one, two, out):
    section = place()[2]
    odd = section % 2 == 1
    one, two = one[...].astype(F32), two[...].astype(F32)
    rows = [turned[i] for i in range(layers)]
    before = jnp.where(section == 0, rows[0], jnp.where(odd, one, two))
    beyond = jnp.where(section == sections - 1, rows[-1], jnp.where(odd, two, one))
    pairs = [(before, before)] + [(row, row) for row in rows] + [(beyond, beyond)]
    chain = [before] + rows + [beyond]
    pairs += list(zip(chain[:-1], chain[1:]))
    out[...] = jnp.zeros_like(out)
    for n, (a, b) in enumerate(pairs):
        out[n : n + 1, :] = jnp.full((1, out.shape[1]), jnp.sum(a * b), F32)


def products(turned, one, two, sections):
    layers = turned.shape[0]
    count = -(-(2 * layers + 3) // 8) * 8
    return pl.pallas_call(
        functools.partial(products_kernel, layers, sections),
        out_shape=jax.ShapeDtypeStruct((count, 128), F32),
        in_specs=[VMEM] * 3,
        out_specs=VMEM,
        compiler_params=params(4),
        cost_estimate=cost(1e6, 1e6),
        name="products",
    )(turned, one, two)


def ratios_kernel(layers, *refs):
    out = refs[-1]
    value = sum(ref[...] for ref in refs[:-1])
    squares = value[: layers + 2]
    chained = value[layers + 2 : 2 * layers + 3]
    ratio = chained / jnp.sqrt(squares[:-1] * squares[1:])
    out[:, 0:1] = ratio[:-1, 0:1]
    out[:, 1:2] = ratio[1:, 0:1]


def ratios(shares, layers):
    return pl.pallas_call(
        functools.partial(ratios_kernel, layers),
        out_shape=jax.ShapeDtypeStruct((layers, 2), F32),
        in_specs=[VMEM] * len(shares),
        out_specs=VMEM,
        compiler_params=params(4),
        cost_estimate=cost(1e4, 1e4),
        name="ratios",
    )(*shares)


def local(activations, projection):
    layers, tok_rows, model = activations.shape
    block, rank = projection.shape
    groups, sections = lax.axis_size("tok"), lax.axis_size("section")
    chips, width = groups // 2, rank // groups
    parts = min(sections, max(1, block // 128))
    deep = block // parts

    acts = activations.reshape(layers * tok_rows, model)
    start = (lax.axis_index("section") & (parts - 1)) * deep
    part = lax.dynamic_slice_in_dim(projection, start, deep, 0)
    mine_part, give_part = deal(part, width)
    got_part = swap(give_part, "tok", 1)
    own = join(mine_part, got_part)

    fetched = {}
    for k in range(1, chips):
        low = k & -k
        fetched[k] = swap(own if k == low else fetched[k ^ low], "tok", 2 * low)

    mine, give = deal(projection, width)
    got = swap(give, "tok", 1)

    order = sorted(fetched, key=lambda k: (bin(k).count("1"), k))
    staged = {}
    for k in [0] + order:
        staged[k] = stage(acts, k, 2 * block)
        staged[k] = (staged[k], swap(staged[k], "tok", 1))

    far = {j: pick(mine, got, parts, j) for j in range(1, parts) if j & (j - 1)}
    both, final = (0, 1), order[-1]
    pieces = {}
    for k in order:
        held = {(0, both): fetched[k]}
        for j in range(1, parts):
            near = j & -j
            if j in far and k in (1, final):
                held[j, both] = swap(far[j], "tok", 2 * k)
            elif j in far and (j ^ near) not in far:
                upper = swap(held[j ^ near, both][:deep], "section", near)
                lower = swap(held[near, both][deep:], "section", j ^ near)
                held[j, (0,)], held[j, (1,)] = upper, lower
            else:
                held[j, both] = swap(fetched[k], "section", j)
        pieces[k] = held

    own_rows = {(None, (0,)): mine, (None, (1,)): got}
    total = project([(staged[0], own_rows)], parts, None, layers, False)

    def held_by(k, kind):
        return {key: piece for key, piece in pieces[k].items() if kind(*key)}

    def is_far(j, which):
        return j in far and len(which) == 2

    near = {k: held_by(k, lambda j, which: j not in far) for k in order}
    passed = [(staged[k], held_by(k, lambda j, which: len(which) == 1)) for k in order]
    distant = [(staged[k], held_by(k, is_far)) for k in order]
    steps = [(f"acc{k}", [(staged[k], near[k])]) for k in order[-2::-1]]
    steps.append((f"acc{final}", [(staged[final], near[final])]))
    steps.append(("last", distant + passed))
    steps = [(name, [group for group in groups_of if group[1]]) for name, groups_of in steps]
    steps = [step for step in steps if step[1]]
    for name, groups_of in steps:
        last = name == steps[-1][0]
        total = project(groups_of, parts, total, layers, last)
    split, sums = total

    split_oth = swap(split, "tok", 1)
    sums_oth = swap(sums, "tok", 1)
    inner = inner_gram(split, layers)
    messages = gram(inner, split, split_oth, sums, sums_oth, layers, chips)
    arrived = [messages[0]]
    for k in reversed(range(1, chips)):
        arrived.append(swap(messages[k].astype(jnp.float16), "tok", 2 * k).astype(F32))
    turned, first, second = finish(arrived, layers, tok_rows * groups)

    route = [(i, i + 1) for i in range(1, sections - 1, 2)]
    second = lax.ppermute(second, "section", route + [(b, a) for a, b in route])
    first = swap(first, "section", 1)
    sketch = upright(turned)
    value = products(turned, first, second, sections)
    value = value + swap(value, "tok", 1)
    if chips <= 4:
        others = []
        for k in reversed(range(1, chips)):
            others.append(swap(value, "tok", 2 * k))
    else:
        mask = 2
        while 2 * mask < groups:
            value = value + swap(value, "tok", mask)
            mask *= 2
        others = [swap(value, "tok", mask)]
    return sketch, ratios([value] + others, layers)


def solution(mesh):
    return jax.shard_map(
        local,
        mesh=mesh,
        in_specs=(P("section", "tok", None), P("tok", None)),
        out_specs=(P("section", None, "tok"), P("section", None)),
        check_vma=False,
    )
```

```python
import functools

import jax
import jax.numpy as jnp
from jax import lax
from jax.experimental import pallas as pl
from jax.experimental.pallas import tpu as pltpu
from jax.sharding import PartitionSpec as P


F32, BF16 = jnp.float32, jnp.bfloat16
VMEM = pl.BlockSpec(memory_space=pltpu.VMEM)
HBM = pl.BlockSpec(memory_space=pltpu.HBM)


def swap(block, axis, mask):
    return lax.ppermute(block, axis, [(i, i ^ mask) for i in range(lax.axis_size(axis))])


def params(mib):
    return pltpu.CompilerParams(vmem_limit_bytes=int(mib * 1024) << 10)


def place():
    tok = lax.axis_index("tok")
    return tok >> 1, tok & 1, lax.axis_index("section")


def cost(flops, moved):
    return pl.CostEstimate(flops=int(flops), bytes_accessed=int(moved), transcendentals=0)


def deal_kernel(width, proj, mine, give):
    core = place()[1]
    rank, half = proj.shape[1], mine.shape[1]
    row = lax.broadcasted_iota(jnp.int32, (rank, half), 0)
    col = lax.broadcasted_iota(jnp.int32, (rank, half), 1)
    first = (col // width) * (2 * width) + col % width
    picks = [
        jnp.where(row == first + side * width, 1.0, 0.0).astype(BF16) for side in (core, 1 - core)
    ]
    for out, pick in zip((mine, give), picks):
        out[...] = jnp.dot(proj[...], pick, preferred_element_type=F32).astype(BF16)


def deal(proj, width):
    rows, rank = proj.shape
    half = jax.ShapeDtypeStruct((rows, rank // 2), BF16)
    return pl.pallas_call(
        functools.partial(deal_kernel, width),
        out_shape=(half, half),
        in_specs=[VMEM],
        out_specs=(VMEM, VMEM),
        compiler_params=params(4),
        cost_estimate=cost(2 * rows * rank * rank, 4 * rows * rank),
        name="deal",
    )(proj)


def stage_kernel(k, source, out, sem):
    deep = out.shape[1]
    columns = pl.ds(pl.multiple_of((place()[0] ^ k) * deep, 128), deep)
    copy = pltpu.make_async_copy(source.at[:, columns], out, sem)
    copy.start()
    copy.wait()


def stage(source, k, deep):
    rows = source.shape[0]
    return pl.pallas_call(
        functools.partial(stage_kernel, k),
        out_shape=jax.ShapeDtypeStruct((rows, deep), BF16),
        in_specs=[HBM],
        out_specs=VMEM,
        scratch_shapes=[pltpu.SemaphoreType.DMA],
        compiler_params=params(3),
        cost_estimate=cost(4e9, 4 * rows * deep),
        name="stage",
    )(source)


def join_kernel(upper, lower, out):
    deep = upper.shape[0]
    out[:deep, :] = upper[...]
    out[deep:, :] = lower[...]


def join(upper, lower):
    deep, half = upper.shape
    return pl.pallas_call(
        join_kernel,
        out_shape=jax.ShapeDtypeStruct((2 * deep, half), BF16),
        in_specs=[VMEM, VMEM],
        out_specs=VMEM,
        compiler_params=params(2),
        cost_estimate=cost(1e6, 8 * deep * half),
        name="join",
    )(upper, lower)


def pick_kernel(parts, j, upper, lower, out):
    deep = out.shape[0] // 2
    rows = pl.ds(pl.multiple_of(((place()[2] % parts) ^ j) * deep, 16), deep)
    out[:deep, :] = upper[rows, :]
    out[deep:, :] = lower[rows, :]


def pick(upper, lower, parts, j):
    rows, half = upper.shape
    return pl.pallas_call(
        functools.partial(pick_kernel, parts, j),
        out_shape=jax.ShapeDtypeStruct((2 * rows // parts, half), BF16),
        in_specs=[VMEM, VMEM],
        out_specs=VMEM,
        compiler_params=params(4),
        cost_estimate=cost(1e6, 8 * rows * half // parts),
        name="pick",
    )(upper, lower)


def project_kernel(groups, parts, started, last, layers, *refs):
    arrays, refs = refs[: 2 * len(groups)], refs[2 * len(groups) :]
    count = sum(len(keys) for keys in groups)
    pieces, refs = refs[:count], refs[count:]
    total = refs[0] if started else None
    outs = refs[started:]
    _, core, section = place()
    part = section % parts
    block = arrays[0].shape[1] // 2
    sides = (core, 1 - core)
    spots = []
    for n, keys in enumerate(groups):
        for j, which in keys:
            for side in which:
                if j is None:
                    spots.append((n, sides[side] * block, block))
                else:
                    at = sides[side] * block + (part ^ j) * (block // parts)
                    spots.append((n, at, block // parts))
    spots = [(n, pl.ds(pl.multiple_of(at, 128), deep)) for n, at, deep in spots]
    weights = jnp.concatenate([piece[...] for piece in pieces], axis=0)
    rows = arrays[0].shape[0] // layers
    left = [
        jnp.concatenate([arrays[2 * n + side][:, columns] for n, columns in spots], axis=1)
        for side in range(2)
    ]
    product = jnp.dot(jnp.concatenate(left, axis=0), weights, preferred_element_type=F32)
    kept = []
    for side in range(2):
        for layer in range(layers):
            span = pl.ds(layer * rows, rows)
            at = (side * layers + layer) * rows
            value = product[at : at + rows]
            if started:
                value = value + total[side, span, :]
            if last:
                kept.append(value)
            else:
                outs[0][side, span, :] = value
    if not last:
        return
    split, sums = outs
    sums[...] = jnp.zeros_like(sums)
    for layer in range(layers):
        values = [kept[layer], kept[layers + layer]]
        column = jnp.sum(values[0] + values[1], axis=0, keepdims=True)
        sums[layer : layer + 1, :] = column
        mean = column / (2 * rows)
        for side in range(2):
            span = pl.ds(layer * rows, rows)
            value = values[side] - mean
            high = value.astype(BF16)
            split[0, side, span, :] = high
            split[1, side, span, :] = (value - high.astype(F32)).astype(BF16)


def project(groups, parts, total, layers, last):
    arrays = [array for acts, _ in groups for array in acts]
    pieces = [piece for _, held in groups for piece in held.values()]
    keys = tuple(tuple(held) for _, held in groups)
    rows, half = arrays[0].shape[0], pieces[0].shape[1]
    deep = sum(piece.shape[0] for piece in pieces)
    if last:
        out_shape = (
            jax.ShapeDtypeStruct((2, 2, rows, half), BF16),
            jax.ShapeDtypeStruct((8, half), F32),
        )
        out_specs = (VMEM, VMEM)
    else:
        out_shape = jax.ShapeDtypeStruct((2, rows, half), F32)
        out_specs = VMEM
    started = [] if total is None else [total]
    return pl.pallas_call(
        functools.partial(project_kernel, keys, parts, len(started), last, layers),
        out_shape=out_shape,
        in_specs=[VMEM] * (len(arrays) + len(pieces) + len(started)),
        out_specs=out_specs,
        compiler_params=params(14 if len(groups) > 1 else 10),
        cost_estimate=cost(4 * rows * deep * half, 4 * rows * deep),
        name="project",
    )(*arrays, *pieces, *started)


def exponent(value):
    top = jnp.max(jnp.abs(value), axis=(0, 1), keepdims=True)
    return jnp.ceil(jnp.log2(jnp.maximum(top, 1e-30))) - 14.0


ALONG_TOKENS = (((0,), (0,)), ((), ()))


def halves(ref, layer, rows, swapped):
    span = pl.ds(layer * rows, rows)
    sides = (1, 0) if swapped else (0, 1)
    return [jnp.concatenate([ref[part, n, span, :] for n in sides], axis=0) for part in range(2)]


def outer(left, right):
    return sum(
        lax.dot_general(left[i], right[j], ALONG_TOKENS, preferred_element_type=F32)
        for i, j in ((0, 0), (0, 1), (1, 0))
    )


def inner_gram_kernel(layers, own, out):
    rows = own.shape[2] // layers
    for layer in range(layers):
        here = halves(own, layer, rows, False)
        out[layer] = outer(here, here)


def inner_gram(own, layers):
    rows, half = own.shape[2:]
    return pl.pallas_call(
        functools.partial(inner_gram_kernel, layers),
        out_shape=jax.ShapeDtypeStruct((layers, half, half), F32),
        in_specs=[VMEM],
        out_specs=VMEM,
        compiler_params=params(6),
        cost_estimate=cost(12 * rows * half * half, 16 * rows * half),
        name="inner_gram",
    )(own)


def gram_kernel(layers, chips, inner, own, oth, own_sums, oth_sums, *outs):
    chip = place()[0]
    half = own.shape[3]
    rows = own.shape[2] // layers
    width = half // chips
    sums = jnp.concatenate([own_sums[...], oth_sums[...]], axis=1)
    tail = []
    for layer in range(layers):
        cross = outer(halves(own, layer, rows, False), halves(oth, layer, rows, True))
        gram = jnp.concatenate([inner[layer], cross], axis=1)
        power = exponent(gram)
        gram = gram * jnp.exp2(-power)
        blocks = [gram[i * width : (i + 1) * width] for i in range(chips)]
        for k, out in enumerate(outs):
            block = blocks[k]
            for i in range(1, chips):
                block = jnp.where(chip == i, blocks[i ^ k], block)
            out[layer * width : (layer + 1) * width, :] = block
        column = sums[layer : layer + 1]
        lift = exponent(column)
        column = column * jnp.exp2(-lift)
        high = column.astype(BF16).astype(F32)
        middle = (column - high).astype(BF16).astype(F32)
        line = jnp.zeros((1, half), F32)
        powers = jnp.concatenate([line + power, line + lift], axis=1)
        tail += [high, middle, column - high - middle, powers]
    for out in outs:
        if len(tail) < tail_rows(layers):
            out[layers * width :, :] = jnp.zeros_like(out[layers * width :, :])
        for n, line in enumerate(tail):
            out[layers * width + n : layers * width + n + 1, :] = line


def tail_rows(layers):
    return -(-4 * layers // 8) * 8


def gram(inner, own, oth, own_sums, oth_sums, layers, chips):
    rows, half = own.shape[2:]
    height = layers * (half // chips) + tail_rows(layers)
    message = jax.ShapeDtypeStruct((height, 2 * half), F32)
    return pl.pallas_call(
        functools.partial(gram_kernel, layers, chips),
        out_shape=(message,) * chips,
        in_specs=[VMEM] * 5,
        out_specs=(VMEM,) * chips,
        compiler_params=params(10),
        cost_estimate=cost(12 * rows * half * half, 16 * rows * half),
        name="gram",
    )(inner, own, oth, own_sums, oth_sums)


def finish_kernel(layers, tokens, *refs):
    messages, (turned, first_out, second_out) = refs[:-3], refs[-3:]
    chips = len(messages)
    chip, _, section = place()
    rank = messages[0].shape[1]
    width = (messages[0].shape[0] - tail_rows(layers)) // layers
    here = lax.broadcasted_iota(jnp.int32, (width, rank), 1)
    here = here == lax.broadcasted_iota(jnp.int32, (width, rank), 0) + chip * width
    kept = []
    for layer in range(layers):
        span = slice(layer * width, (layer + 1) * width)
        at = layers * width + 4 * layer
        value, sums = 0.0, []
        for message in messages:
            line = [message[at + n : at + n + 1, :] for n in range(4)]
            scale = jnp.exp2(line[3])
            value = value + message[span, :] * scale[:, :1]
            sums.append((line[0] + line[1] + line[2]) * scale[:, rank - 1 :])
        mean = sum(sums) / tokens
        for total in sums:
            drift = total / (tokens // chips) - mean
            lifted = jnp.sum(jnp.where(here, drift, 0.0), axis=1, keepdims=True)
            value = value + (tokens // chips) * lifted * drift
        turned[layer] = value
        kept.append(value)
    odd = section % 2 == 1
    first_out[...] = jnp.where(odd, kept[0], kept[-1]).astype(BF16)
    second_out[...] = jnp.where(odd, kept[-1], kept[0]).astype(BF16)


def finish(messages, layers, tokens):
    height, rank = messages[0].shape
    width = (height - tail_rows(layers)) // layers
    edge = jax.ShapeDtypeStruct((width, rank), BF16)
    return pl.pallas_call(
        functools.partial(finish_kernel, layers, tokens),
        out_shape=(
            jax.ShapeDtypeStruct((layers, width, rank), F32),
            edge,
            edge,
        ),
        in_specs=[VMEM] * len(messages),
        out_specs=(VMEM,) * 3,
        compiler_params=params(6),
        cost_estimate=cost(1e6, 2e6),
        name="finish",
    )(*messages)


def upright_kernel(turned, sketch):
    core = place()[1]
    layers, width, rank = turned.shape
    for layer in range(layers):
        flipped = turned[layer].T
        for i in range(rank // (2 * width)):
            for side in range(2):
                at = side * (rank // 2) + i * width
                to = 2 * width * i + width * (core if side == 0 else 1 - core)
                rows = pl.ds(pl.multiple_of(to, 8), width)
                sketch[layer, rows, :] = flipped[at : at + width]


def upright(turned):
    layers, width, rank = turned.shape
    return pl.pallas_call(
        upright_kernel,
        out_shape=jax.ShapeDtypeStruct((layers, rank, width), F32),
        in_specs=[VMEM],
        out_specs=VMEM,
        compiler_params=params(6),
        cost_estimate=cost(1e6, 2e6),
        name="upright",
    )(turned)


def products_kernel(layers, sections, turned, one, two, out):
    section = place()[2]
    odd = section % 2 == 1
    one, two = one[...].astype(F32), two[...].astype(F32)
    rows = [turned[i] for i in range(layers)]
    before = jnp.where(section == 0, rows[0], jnp.where(odd, one, two))
    beyond = jnp.where(section == sections - 1, rows[-1], jnp.where(odd, two, one))
    pairs = [(before, before)] + [(row, row) for row in rows] + [(beyond, beyond)]
    chain = [before] + rows + [beyond]
    pairs += list(zip(chain[:-1], chain[1:]))
    out[...] = jnp.zeros_like(out)
    for n, (a, b) in enumerate(pairs):
        out[n : n + 1, :] = jnp.full((1, out.shape[1]), jnp.sum(a * b), F32)


def products(turned, one, two, sections):
    layers = turned.shape[0]
    count = -(-(2 * layers + 3) // 8) * 8
    return pl.pallas_call(
        functools.partial(products_kernel, layers, sections),
        out_shape=jax.ShapeDtypeStruct((count, 128), F32),
        in_specs=[VMEM] * 3,
        out_specs=VMEM,
        compiler_params=params(4),
        cost_estimate=cost(1e6, 1e6),
        name="products",
    )(turned, one, two)


def ratios_kernel(layers, *refs):
    out = refs[-1]
    value = sum(ref[...] for ref in refs[:-1])
    squares = value[: layers + 2]
    chained = value[layers + 2 : 2 * layers + 3]
    ratio = chained / jnp.sqrt(squares[:-1] * squares[1:])
    out[:, 0:1] = ratio[:-1, 0:1]
    out[:, 1:2] = ratio[1:, 0:1]


def ratios(shares, layers):
    return pl.pallas_call(
        functools.partial(ratios_kernel, layers),
        out_shape=jax.ShapeDtypeStruct((layers, 2), F32),
        in_specs=[VMEM] * len(shares),
        out_specs=VMEM,
        compiler_params=params(4),
        cost_estimate=cost(1e4, 1e4),
        name="ratios",
    )(*shares)


def local(activations, projection):
    layers, tok_rows, model = activations.shape
    block, rank = projection.shape
    groups, sections = lax.axis_size("tok"), lax.axis_size("section")
    chips, width = groups // 2, rank // groups
    parts = min(sections, max(1, block // 128))
    deep = block // parts

    acts = activations.reshape(layers * tok_rows, model)
    start = (lax.axis_index("section") & (parts - 1)) * deep
    part = lax.dynamic_slice_in_dim(projection, start, deep, 0)
    mine_part, give_part = deal(part, width)
    got_part = swap(give_part, "tok", 1)
    own = join(mine_part, got_part)

    fetched = {}
    for k in range(1, chips):
        low = k & -k
        fetched[k] = swap(own if k == low else fetched[k ^ low], "tok", 2 * low)

    mine, give = deal(projection, width)
    got = swap(give, "tok", 1)

    order = sorted(fetched, key=lambda k: (bin(k).count("1"), k))
    staged = {}
    for k in [0] + order:
        staged[k] = stage(acts, k, 2 * block)
        staged[k] = (staged[k], swap(staged[k], "tok", 1))

    far = {j: pick(mine, got, parts, j) for j in range(1, parts) if j & (j - 1)}
    both, final = (0, 1), order[-1]
    pieces = {}
    for k in order:
        held = {(0, both): fetched[k]}
        for j in range(1, parts):
            near = j & -j
            if j in far and k in (1, final):
                held[j, both] = swap(far[j], "tok", 2 * k)
            elif j in far and (j ^ near) not in far:
                upper = swap(held[j ^ near, both][:deep], "section", near)
                lower = swap(held[near, both][deep:], "section", j ^ near)
                held[j, (0,)], held[j, (1,)] = upper, lower
            else:
                held[j, both] = swap(fetched[k], "section", j)
        pieces[k] = held

    own_rows = {(None, (0,)): mine, (None, (1,)): got}
    total = project([(staged[0], own_rows)], parts, None, layers, False)

    def held_by(k, kind):
        return {key: piece for key, piece in pieces[k].items() if kind(*key)}

    def is_far(j, which):
        return j in far and len(which) == 2

    near = {k: held_by(k, lambda j, which: j not in far) for k in order}
    passed = [(staged[k], held_by(k, lambda j, which: len(which) == 1)) for k in order]
    distant = [(staged[k], held_by(k, is_far)) for k in order]
    steps = [(f"acc{k}", [(staged[k], near[k])]) for k in order[-2::-1]]
    steps.append((f"acc{final}", [(staged[final], near[final])]))
    steps.append(("last", distant + passed))
    steps = [(name, [group for group in groups_of if group[1]]) for name, groups_of in steps]
    steps = [step for step in steps if step[1]]
    for name, groups_of in steps:
        last = name == steps[-1][0]
        total = project(groups_of, parts, total, layers, last)
    split, sums = total

    split_oth = swap(split, "tok", 1)
    sums_oth = swap(sums, "tok", 1)
    inner = inner_gram(split, layers)
    messages = gram(inner, split, split_oth, sums, sums_oth, layers, chips)
    arrived = [messages[0]]
    for k in reversed(range(1, chips)):
        arrived.append(swap(messages[k].astype(jnp.float16), "tok", 2 * k).astype(F32))
    turned, first, second = finish(arrived, layers, tok_rows * groups)

    route = [(i, i + 1) for i in range(1, sections - 1, 2)]
    second = lax.ppermute(second, "section", route + [(b, a) for a, b in route])
    first = swap(first, "section", 1)
    sketch = upright(turned)
    value = products(turned, first, second, sections)
    value = value + swap(value, "tok", 1)
    if chips <= 4:
        others = []
        for k in reversed(range(1, chips)):
            others.append(swap(value, "tok", 2 * k))
    else:
        mask = 2
        while 2 * mask < groups:
            value = value + swap(value, "tok", mask)
            mask *= 2
        others = [swap(value, "tok", mask)]
    return sketch, ratios([value] + others, layers)


def solution(mesh):
    return jax.shard_map(
        local,
        mesh=mesh,
        in_specs=(P("section", "tok", None), P("tok", None)),
        out_specs=(P("section", None, "tok"), P("section", None)),
        check_vma=False,
    )
```
